256 devices in a mesh: gx: 64 (over x, z_hi, y, core), gy: 4 (over z_lo).
Axes of the slice: x: 4, y: 4, z: 8 (z_hi: 2, z_lo: 4; z = z_hi * 4 + z_lo), core: 2. Of those that a mesh axis runs over, the one named last changes fastest.
Arguments:
- adjoint: float32 [9, 256, 128, 512], P(None, 'gx', 'gy'), may hold values from -6 to 6
- buoyancy: float32 [256, 128, 512], P('gx', 'gy'), may hold values from 0.5 to 2
- lame_lambda: float32 [256, 128, 512], P('gx', 'gy'), may hold values from 0.5 to 2
- shear_mu: float32 [256, 128, 512], P('gx', 'gy'), may hold values from 0.3 to 1.2
- packed: int32 [64, 64, 4, 12, 256], P('gx', None, 'gy'), may hold values from -2147483648 to 2147483646
- scales: float32 [64, 64, 4, 12], P('gx', None, 'gy'), may hold values from 0.005 to 0.05
- perm: int32 [64, 64], P('gx'), may hold values from 0 to 63, each once within a row
Outputs:
- adjoint_out: float32 [9, 256, 128, 512], P(None, 'gx', 'gy')
- gradients: float32 [2, 256, 128, 512], P(None, 'gx', 'gy')
The draws below stay inside these ranges and needn't reach their ends.
Inputs may be any that keep to these rules, and one draw needn't show every extreme that they name: Each row of perm names every number 0 to 63 once. The words of packed are stored inputs and may cross devices as they are, four signed bytes to a word; only values that a program computes travel in float32.
All inputs are finite; a program needn't handle non-finite values.
Results may differ from the reference program's by a relative error of at most 0.0003.
Values sent between devices are 32-bit elements; how exact they have to be, the bound alone decides.
No kernel may reach another device: no remote copies, remote signals or barrier semaphores. Data moves between devices by JAX's collectives and lax.ppermute only.
A program may use at most 128 MiB of HBM per device.

```python
import math
import jax
import jax.numpy as jnp
from jax import lax

CX = 4
CY = 32
CZ = 512
STEPS = 2
COMP = 12
OWNERS = 64
SEGW = 256
NX = 256
NY = 128
NZ = 512
N_GY = 4


def place_ends(values, key, low, top_value):
    longest = values.shape.index(max(values.shape))
    spots = []
    for shift in (0, 1):
        where = [jax.random.randint(jax.random.fold_in(key, axis), (), 0, length) for axis, length in enumerate(values.shape)]
        where[longest] = (where[longest] + shift) % values.shape[longest]
        spots.append(tuple(where))
    return values.at[spots[0]].set(low).at[spots[1]].set(top_value)


def steps_of(stream_key, extent, cuts, low, top_value):
    loudness = 1.0
    for position, parts in cuts:
        draws = jax.random.uniform(jax.random.fold_in(jax.random.fold_in(stream_key, 6), position), (parts,), jnp.float32, low / len(cuts), top_value / len(cuts))
        loudness = loudness * jnp.repeat(jnp.exp(draws), extent[position] // parts).reshape((-1,) + (1,) * (len(extent) - 1 - position))
    return loudness


def normal_values(own_key, shape, spread, bound, cuts=(), kind=jnp.bfloat16):
    values = jax.random.normal(own_key, shape, jnp.float32) * spread
    if len(cuts) > 0:
        values = steps_of(own_key, shape, cuts, -0.22, 0.18) * values
    return jnp.clip(values, min=-bound, max=bound).astype(kind)


def setup_inputs(seed: int = 0) -> dict:
    keys = jax.random.split(jax.random.key(seed), 8)
    adjoint = normal_values(keys[0], (9, NX, NY, NZ), 1.0, 6.0, ((1, 64), (2, 4)), jnp.float32)
    buoyancy = jnp.clip(jnp.exp(math.log(2.0) - 1.3862944 * jax.random.uniform(keys[1], (NX, NY, NZ), jnp.float32) ** steps_of(keys[1], (NX, NY, NZ), ((0, 64), (1, 4)), -0.2, 0.2)), 0.5, 2.0)
    lame_lambda = jnp.clip(jnp.exp(math.log(2.0) - 1.3862944 * jax.random.uniform(keys[2], (NX, NY, NZ), jnp.float32) ** steps_of(keys[2], (NX, NY, NZ), ((0, 64), (1, 4)), -0.2, 0.2)), 0.5, 2.0)
    shear_mu = jnp.clip(jnp.exp(math.log(1.2) - 1.3862944 * jax.random.uniform(keys[3], (NX, NY, NZ), jnp.float32) ** steps_of(keys[3], (NX, NY, NZ), ((0, 64), (1, 4)), -0.2, 0.2)), 0.3, 1.2)
    packed = place_ends(jax.random.randint(keys[4], (OWNERS, OWNERS, N_GY, COMP, SEGW), -2147483648, 2147483647), jax.random.fold_in(keys[4], 1), -2147483648, 2147483646).astype(jnp.int32)
    scales = jnp.clip(jnp.exp(math.log(0.05) - 2.3025851 * jax.random.uniform(keys[5], (OWNERS, OWNERS, N_GY, COMP), jnp.float32) ** steps_of(keys[5], (OWNERS, OWNERS, N_GY, COMP), ((0, 64), (2, 4)), -0.2, 0.2)), 0.005, 0.05)
    perm = jax.vmap(lambda own: jax.random.permutation(own, OWNERS))(jax.random.split(keys[6], OWNERS)).reshape((OWNERS, OWNERS)).astype(jnp.int32)
    return dict(adjoint=adjoint, buoyancy=buoyancy, lame_lambda=lame_lambda, shear_mu=shear_mu, packed=packed, scales=scales, perm=perm)


courant = 0.15


def unpack(words):
    low = (words & 255) - 128
    middle = (jnp.right_shift(words, 8) & 255) - 128
    high = (jnp.right_shift(words, 16) & 255) - 128
    topmost = jnp.right_shift(words, 24)
    return jnp.concatenate([low, middle, high, topmost], axis=-1).astype(jnp.float32)


def inverse_order(row):
    count = row.shape[0]
    slots = jnp.arange(count, dtype=jnp.int32)
    hits = (row[None, :] == slots[:, None]).astype(jnp.int32)
    return jnp.sum(hits * slots[None, :], axis=1).astype(jnp.int32)


def forward_field(packed, scales, perm):
    comp = packed.shape[3]
    by_owner = jnp.swapaxes(packed, 0, 1)
    factors = jnp.swapaxes(scales, 0, 1)

    def one_owner(items):
        words, factor, row = items
        blocks = unpack(words) * factor[..., None]
        ordered = jnp.take(blocks, inverse_order(row), axis=0)
        return jnp.transpose(ordered, (2, 1, 0, 3)).reshape(comp, N_GY, CX, CY, CZ)

    whole_field = lax.map(one_owner, (by_owner, factors, perm))
    whole_field = jnp.transpose(whole_field, (1, 0, 3, 2, 4, 5))
    return whole_field.reshape(comp, NX, NY, NZ)


def step_ahead(field, axis):
    count = field.shape[axis]
    widths = [(0, 0)] * field.ndim
    widths[axis] = (0, 1)
    return jnp.pad(lax.slice_in_dim(field, 1, count, axis=axis), widths)


def step_behind(field, axis):
    count = field.shape[axis]
    widths = [(0, 0)] * field.ndim
    widths[axis] = (1, 0)
    return jnp.pad(lax.slice_in_dim(field, 0, count - 1, axis=axis), widths)


def diff_ahead(field, axis):
    return step_ahead(field, axis) - field


def diff_behind(field, axis):
    return field - step_behind(field, axis)


def move_velocity(velocity, stress, buoyancy):
    scaled = courant * buoyancy
    return [
        velocity[0] - scaled * (diff_ahead(stress[0], 0) + diff_behind(stress[3], 1) + diff_behind(stress[4], 2)),
        velocity[1] - scaled * (diff_behind(stress[3], 0) + diff_ahead(stress[1], 1) + diff_behind(stress[5], 2)),
        velocity[2] - scaled * (diff_behind(stress[4], 0) + diff_behind(stress[5], 1) + diff_ahead(stress[2], 2)),
    ]


def strains(velocity):
    return [
        diff_behind(velocity[0], 0),
        diff_behind(velocity[1], 1),
        diff_behind(velocity[2], 2),
        diff_ahead(velocity[0], 1) + diff_ahead(velocity[1], 0),
        diff_ahead(velocity[0], 2) + diff_ahead(velocity[2], 0),
        diff_ahead(velocity[1], 2) + diff_ahead(velocity[2], 1),
    ]


def move_stress(stress, strain, lame_lambda, shear_mu):
    trace = strain[0] + strain[1] + strain[2]
    result = []
    for index in range(3):
        result.append(stress[index] - courant * (lame_lambda * trace + 2.0 * shear_mu * strain[index]))
    for index in range(3, 6):
        result.append(stress[index] - courant * shear_mu * strain[index])
    return result


def reference(adjoint, buoyancy, lame_lambda, shear_mu, packed, scales, perm):
    forward = forward_field(packed, scales, perm)
    velocity = [adjoint[index] for index in range(3)]
    stress = [adjoint[index] for index in range(3, 9)]
    grad_lambda = jnp.zeros(buoyancy.shape, jnp.float32)
    grad_mu = jnp.zeros(buoyancy.shape, jnp.float32)
    for step in range(STEPS):
        velocity = move_velocity(velocity, stress, buoyancy)
        strain = strains(velocity)
        stress = move_stress(stress, strain, lame_lambda, shear_mu)
        stored = [forward[6 * step + index] for index in range(6)]
        trace = strain[0] + strain[1] + strain[2]
        grad_lambda = grad_lambda + trace * (stored[0] + stored[1] + stored[2])
        grad_mu = grad_mu + 2.0 * (strain[0] * stored[0] + strain[1] * stored[1] + strain[2] * stored[2])
        grad_mu = grad_mu + strain[3] * stored[3] + strain[4] * stored[4] + strain[5] * stored[5]
    return jnp.stack(velocity + stress), jnp.stack([grad_lambda, grad_mu])
```

```python
import jax
import jax.numpy as jnp
from jax import lax
from jax.experimental import pallas as pl
from jax.experimental.pallas import tpu as pltpu
from jax.sharding import PartitionSpec as P

courant = 0.15
FACTOR_UP = 2.0**35
FACTOR_DOWN = 2.0**-35
F32 = jnp.float32
ANY = pl.BlockSpec(memory_space=pl.ANY)
VMEM = pl.BlockSpec(memory_space=pltpu.VMEM)


def below_y(field, row):
    y = lax.broadcasted_iota(jnp.int32, field.shape, 0)
    return jnp.where(y == 0, row, pltpu.roll(field, 1, 0))


def above_y(field, row):
    count = field.shape[0]
    y = lax.broadcasted_iota(jnp.int32, field.shape, 0)
    return jnp.where(y == count - 1, row, pltpu.roll(field, count - 1, 0))


def below_z(field):
    z = lax.broadcasted_iota(jnp.int32, field.shape, 1)
    return jnp.where(z == 0, 0.0, pltpu.roll(field, 1, 1))


def above_z(field):
    count = field.shape[1]
    z = lax.broadcasted_iota(jnp.int32, field.shape, 1)
    return jnp.where(z == count - 1, 0.0, pltpu.roll(field, count - 1, 1))


def velocity_plane(vel, scaled, sxx, sxx_next, syy, syy_row, szz, sxy, sxy_prior, sxy_row, sxz, sxz_prior, syz, syz_row):
    vx, vy, vz = vel
    vx = vx - scaled * (sxx_next - sxx + (sxy - below_y(sxy, sxy_row)) + (sxz - below_z(sxz)))
    vy = vy - scaled * (sxy - sxy_prior + (above_y(syy, syy_row) - syy) + (syz - below_z(syz)))
    vz = vz - scaled * (sxz - sxz_prior + (syz - below_y(syz, syz_row)) + (above_z(szz) - szz))
    return vx, vy, vz


def strain_plane(vx, vx_prior, vx_row, vy, vy_next, vy_row, vz, vz_next, vz_row):
    exx = vx - vx_prior
    eyy = vy - below_y(vy, vy_row)
    ezz = vz - below_z(vz)
    exy = (above_y(vx, vx_row) - vx) + (vy_next - vy)
    exz = (above_z(vx) - vx) + (vz_next - vz)
    eyz = (above_z(vy) - vy) + (above_y(vz, vz_row) - vz)
    return exx, eyy, ezz, exy, exz, eyz


def stress_plane(stress, strain, lam, mu):
    trace = strain[0] + strain[1] + strain[2]
    direct = [stress[k] - courant * (lam * trace + 2.0 * mu * strain[k]) for k in range(3)]
    shear = [stress[k] - courant * mu * strain[k] for k in range(3, 6)]
    return direct + shear


def prepare(adj, lam, mu, packed, scales, message, to_next_x, to_prior_x, to_next_y, to_prior_y, words, rows, sems, word_sem):
    cells_x = adj.shape[1]
    cells_y = adj.shape[2]
    count = scales.shape[0]
    per = packed.shape[0] // count
    word_copy = pltpu.make_async_copy(packed, words, word_sem)
    word_copy.start()
    plans = [
        (adj.at[6, cells_x - 1], to_next_x.at[0]),
        (adj.at[7, cells_x - 1], to_next_x.at[1]),
        (mu.at[cells_x - 1], to_next_x.at[2]),
        (adj.at[3, 0], to_prior_x.at[0]),
        (lam.at[0], to_prior_x.at[1]),
        (mu.at[0], to_prior_x.at[2]),
        (adj.at[6, :, pl.ds(cells_y - 8, 8)], rows.at[0]),
        (adj.at[8, :, pl.ds(cells_y - 8, 8)], rows.at[1]),
        (mu.at[:, pl.ds(cells_y - 8, 8)], rows.at[2]),
        (adj.at[4, :, pl.ds(0, 8)], rows.at[3]),
        (lam.at[:, pl.ds(0, 8)], rows.at[4]),
        (mu.at[:, pl.ds(0, 8)], rows.at[5]),
    ]
    copies = [pltpu.make_async_copy(source, target, sems.at[n]) for n, (source, target) in enumerate(plans)]
    for copy in copies:
        copy.start()
    factor = (scales[...] * FACTOR_UP).astype(jnp.int32)
    message[pl.ds(per, count, stride=per + 1), :] = jnp.pad(factor, ((0, 0), (0, 128 - factor.shape[1])))
    for copy in copies:
        copy.wait()
    for k in range(3):
        for x in range(cells_x):
            to_next_y[k, x : x + 1, :] = rows[k, x, 7:8, :]
            to_prior_y[k, x : x + 1, :] = rows[3 + k, x, 0:1, :]
    word_copy.wait()
    for r in range(per):
        message[pl.ds(r, count, stride=per + 1), :] = words[pl.ds(r, count, stride=per), :]


def first_velocity(adj, buoy, prior_x, next_x, prior_y, next_y, v, to_next_x, to_prior_x, to_next_y, to_prior_y, to_lower, to_upper):
    cells_x = adj.shape[1]
    cells_y = adj.shape[2]
    for x in range(cells_x):
        sxy_prior = adj[6, x - 1] if x > 0 else prior_x[0]
        sxz_prior = adj[7, x - 1] if x > 0 else prior_x[1]
        sxx_next = adj[3, x + 1] if x < cells_x - 1 else next_x[0]
        new = velocity_plane(
            (adj[0, x], adj[1, x], adj[2, x]), courant * buoy[x], adj[3, x], sxx_next, adj[4, x], next_y[0, x : x + 1], adj[5, x],
            adj[6, x], sxy_prior, prior_y[0, x : x + 1], adj[7, x], sxz_prior, adj[8, x], prior_y[1, x : x + 1],
        )
        for k in range(3):
            v[k, x] = new[k]
            to_next_y[k, x : x + 1, :] = new[k][cells_y - 1 :, :]
            to_prior_y[k, x : x + 1, :] = new[k][0:1, :]
            if x == cells_x - 1:
                to_next_x[k] = new[k]
            if x == 0:
                to_prior_x[k] = new[k]
        if x == cells_x - 1:
            to_lower[...] = new[0][0:1, :]
        if x == 0:
            to_upper[...] = new[1][cells_y - 1 :, :]


def middle(
    adj, buoy, lam, mu, s_prior_x, s_next_x, s_prior_y, s_next_y, v, last_y, first_y,
    v_prior_x, v_next_x, v_prior_y, v_next_y, vx_corner, vy_corner,
    v_new, stress, strain, to_next_x, to_prior_x, to_next_y, to_prior_y,
):
    cells_x = adj.shape[1]
    cells_y = adj.shape[2]
    last = cells_x - 1
    vx_m, vy_m, vz_m = v_prior_x[0], v_prior_x[1], v_prior_x[2]
    vx_n, vy_n, vz_n = v_next_x[0], v_next_x[1], v_next_x[2]
    exx = vx_n - v[0, last]
    trace = exx + (vy_n - below_y(vy_n, vy_corner[...])) + (vz_n - below_z(vz_n))
    sxx_next = s_next_x[0] - courant * (s_next_x[1] * trace + 2.0 * s_next_x[2] * exx)
    exy = (above_y(vx_m, vx_corner[...]) - vx_m) + (v[1, 0] - vy_m)
    exz = (above_z(vx_m) - vx_m) + (v[2, 0] - vz_m)
    sxy_prior = s_prior_x[0] - courant * s_prior_x[2] * exy
    sxz_prior = s_prior_x[1] - courant * s_prior_x[2] * exz
    above = v_next_y[0]
    exx = above - jnp.concatenate([vx_corner[...], above[:last]], axis=0)
    eyy = v_next_y[1] - last_y[1]
    trace = exx + eyy + (v_next_y[2] - below_z(v_next_y[2]))
    syy_rows = s_next_y[0] - courant * (s_next_y[1] * trace + 2.0 * s_next_y[2] * eyy)
    under = v_prior_y[1]
    exy = (first_y[0] - v_prior_y[0]) + (jnp.concatenate([under[1:], vy_corner[...]], axis=0) - under)
    eyz = (above_z(under) - under) + (first_y[2] - v_prior_y[2])
    sxy_rows = s_prior_y[0] - courant * s_prior_y[2] * exy
    syz_rows = s_prior_y[1] - courant * s_prior_y[2] * eyz
    for x in range(cells_x):
        e = strain_plane(
            v[0, x], v[0, x - 1] if x > 0 else vx_m, v_next_y[0, x : x + 1],
            v[1, x], v[1, x + 1] if x < last else vy_n, v_prior_y[1, x : x + 1],
            v[2, x], v[2, x + 1] if x < last else vz_n, v_next_y[2, x : x + 1],
        )
        s = stress_plane([adj[3 + k, x] for k in range(6)], e, lam[x], mu[x])
        for k in range(6):
            strain[k, x] = e[k]
            stress[k, x] = s[k]
    for x in range(cells_x):
        new = velocity_plane(
            (v[0, x], v[1, x], v[2, x]), courant * buoy[x],
            stress[0, x], stress[0, x + 1] if x < last else sxx_next, stress[1, x], syy_rows[x : x + 1], stress[2, x],
            stress[3, x], stress[3, x - 1] if x > 0 else sxy_prior, sxy_rows[x : x + 1],
            stress[4, x], stress[4, x - 1] if x > 0 else sxz_prior, stress[5, x], syz_rows[x : x + 1],
        )
        for k in range(3):
            v_new[k, x] = new[k]
        to_next_y[0, x : x + 1, :] = new[1][cells_y - 1 :, :]
        to_prior_y[0, x : x + 1, :] = new[0][0:1, :]
        to_prior_y[1, x : x + 1, :] = new[2][0:1, :]
        if x == last:
            to_next_x[0] = new[0]
        if x == 0:
            to_prior_x[0] = new[1]
            to_prior_x[1] = new[2]


def second_stress(v, stress, lam, mu, prior_x, next_x, prior_y, next_y, out, strain):
    cells_x = v.shape[1]
    last = cells_x - 1
    for x in range(cells_x):
        e = strain_plane(
            v[0, x], v[0, x - 1] if x > 0 else prior_x[0], next_y[0, x : x + 1],
            v[1, x], v[1, x + 1] if x < last else next_x[0], prior_y[0, x : x + 1],
            v[2, x], v[2, x + 1] if x < last else next_x[1], next_y[1, x : x + 1],
        )
        s = stress_plane([stress[k, x] for k in range(6)], e, lam[x], mu[x])
        for k in range(3):
            out[k, x] = v[k, x]
        for k in range(6):
            strain[k, x] = e[k]
            out[3 + k, x] = s[k]


def gradients(message, perm, strain1, strain2, out):
    count = perm.shape[1]
    per = message.shape[0] // count
    cells_x, cells_y, cells_z = strain1.shape[1:]
    rows = cells_x * cells_y
    both = jnp.concatenate([perm[...], perm[...]], axis=1)
    r = lax.broadcasted_iota(jnp.int32, (rows, 2 * count), 0)
    k = lax.broadcasted_iota(jnp.int32, (rows, 2 * count), 1)
    mine = both == lax.shift_right_logical(r, 1)
    half = (k >= count) == ((r & 1) == 1)
    pick = jnp.where(mine & half, 1.0, 0.0).astype(jnp.bfloat16)
    pick_factor = jnp.where(mine & (k < count), 1.0, 0.0)
    factor = message[pl.ds(per - 1, count, stride=per), :].astype(F32) * FACTOR_DOWN
    factor = jnp.concatenate([factor, jnp.zeros_like(factor)], axis=0)
    factor = lax.dot(pick_factor, factor, precision=lax.Precision.HIGHEST, preferred_element_type=F32)

    def forward(c):
        w = [message[pl.ds(2 * c + t, count, stride=per), :] for t in range(2)]
        byte = [lambda w: w & 255, lambda w: lax.shift_right_logical(w, 8) & 255, lambda w: lax.shift_right_logical(w, 16) & 255]
        parts = [[(f(v) - 128) for v in w] for f in byte] + [[lax.shift_right_arithmetic(v, 24) for v in w]]
        parts = [[v.astype(F32).astype(jnp.bfloat16) for v in p] for p in parts]
        low = jnp.concatenate(parts[0] + parts[1], axis=1)
        high = jnp.concatenate(parts[2] + parts[3], axis=1)
        table = jnp.concatenate([low, high], axis=0)
        picked = lax.dot(pick, table, preferred_element_type=F32)
        return picked * factor[:, c : c + 1]

    grad_lambda = None
    grad_mu = None
    for step, strain in enumerate((strain1, strain2)):
        f = [forward(6 * step + n) for n in range(6)]
        e = [strain[n].reshape(rows, cells_z) for n in range(6)]
        add_lambda = (e[0] + e[1] + e[2]) * (f[0] + f[1] + f[2])
        add_mu = 2.0 * (e[0] * f[0] + e[1] * f[1] + e[2] * f[2])
        grad_lambda = add_lambda if step == 0 else grad_lambda + add_lambda
        grad_mu = add_mu if step == 0 else grad_mu + add_mu
        grad_mu = grad_mu + e[3] * f[3] + e[4] * f[4] + e[5] * f[5]
    out[0] = grad_lambda.reshape(cells_x, cells_y, cells_z)
    out[1] = grad_mu.reshape(cells_x, cells_y, cells_z)


def on_device(adjoint, buoyancy, lame_lambda, shear_mu, packed, scales, perm):
    cells_x, cells_y, cells_z = buoyancy.shape
    owners, comp, width = packed.shape[1], packed.shape[3], packed.shape[4]
    per = comp * width // 128

    def shape(*dims):
        return jax.ShapeDtypeStruct(dims, F32)

    plane = (cells_y, cells_z)
    line = (cells_x, cells_z)

    count_x = lax.axis_size("gx")
    count_y = lax.axis_size("gy")

    def along(value, step_x, step_y):
        pairs = [
            (x * count_y + y, (x + step_x) * count_y + y + step_y)
            for x in range(count_x)
            for y in range(count_y)
            if 0 <= x + step_x < count_x and 0 <= y + step_y < count_y
        ]
        return lax.ppermute(value, ("gx", "gy"), pairs)

    words = packed.reshape(owners * per, 128)
    message, nx, px, ny, py = pl.pallas_call(
        prepare,
        out_shape=(
            jax.ShapeDtypeStruct((owners * (per + 1), 128), jnp.int32),
            shape(3, *plane), shape(3, *plane), shape(3, *line), shape(3, *line),
        ),
        in_specs=[ANY, ANY, ANY, ANY, VMEM],
        out_specs=(VMEM,) * 5,
        scratch_shapes=[
            pltpu.VMEM((owners * per, 128), jnp.int32),
            pltpu.VMEM((6, cells_x, 8, cells_z), F32),
            pltpu.SemaphoreType.DMA((12,)),
            pltpu.SemaphoreType.DMA,
        ],
        name="prepare",
    )(adjoint, lame_lambda, shear_mu, words, scales.reshape(owners, comp))
    s_prior_x = along(nx, 1, 0)
    s_next_x = along(px, -1, 0)
    s_prior_y = along(ny, 0, 1)
    s_next_y = along(py, 0, -1)
    message = lax.all_to_all(message.reshape(owners, per + 1, 1, 128), "gx", split_axis=0, concat_axis=0, tiled=True)
    message = message.reshape(owners * (per + 1), 128)

    v, nx, px, ny, py, low, up = pl.pallas_call(
        first_velocity,
        out_shape=(
            shape(3, cells_x, *plane), shape(3, *plane), shape(3, *plane), shape(3, *line), shape(3, *line),
            shape(1, cells_z), shape(1, cells_z),
        ),
        in_specs=[VMEM] * 6,
        out_specs=(VMEM,) * 7,
        name="first_velocity",
    )(adjoint, buoyancy, s_prior_x, s_next_x, s_prior_y, s_next_y)
    v_prior_x = along(nx, 1, 0)
    v_next_x = along(px, -1, 0)
    v_prior_y = along(ny, 0, 1)
    v_next_y = along(py, 0, -1)
    vx_corner = along(low, 1, -1)
    vy_corner = along(up, -1, 1)

    v2, stress, strain1, nx, px, ny2, py2 = pl.pallas_call(
        middle,
        out_shape=(
            shape(3, cells_x, *plane), shape(6, cells_x, *plane), shape(6, cells_x, *plane),
            shape(1, *plane), shape(2, *plane), shape(1, *line), shape(2, *line),
        ),
        in_specs=[VMEM] * 17,
        out_specs=(VMEM,) * 7,
        name="middle",
    )(
        adjoint, buoyancy, lame_lambda, shear_mu, s_prior_x, s_next_x, s_prior_y, s_next_y, v, ny, py,
        v_prior_x, v_next_x, v_prior_y, v_next_y, vx_corner, vy_corner,
    )
    w_prior_x = along(nx, 1, 0)
    w_next_x = along(px, -1, 0)
    w_prior_y = along(ny2, 0, 1)
    w_next_y = along(py2, 0, -1)

    adjoint_out, strain2 = pl.pallas_call(
        second_stress,
        out_shape=(shape(*adjoint.shape), shape(6, cells_x, *plane)),
        in_specs=[VMEM] * 8,
        out_specs=(VMEM,) * 2,
        name="second_stress",
    )(v2, stress, lame_lambda, shear_mu, w_prior_x, w_next_x, w_prior_y, w_next_y)

    grads = pl.pallas_call(
        gradients,
        out_shape=shape(2, cells_x, *plane),
        in_specs=[VMEM] * 4,
        out_specs=VMEM,
        name="gradients",
    )(message, perm, strain1, strain2)
    return adjoint_out, grads


def solution(mesh):
    return jax.shard_map(
        on_device,
        mesh=mesh,
        in_specs=(
            P(None, "gx", "gy", None),
            P("gx", "gy", None),
            P("gx", "gy", None),
            P("gx", "gy", None),
            P("gx", None, "gy", None, None),
            P("gx", None, "gy", None),
            P("gx", None),
        ),
        out_specs=(P(None, "gx", "gy", None), P(None, "gx", "gy", None)),
        check_vma=False,
    )
```

```python
import jax
import jax.numpy as jnp
from jax import lax
from jax.experimental import pallas as pl
from jax.experimental.pallas import tpu as pltpu
from jax.sharding import PartitionSpec as P


courant = 0.15
FACTOR_UP = 2.0**35
FACTOR_DOWN = 2.0**-35
F32 = jnp.float32
ANY = pl.BlockSpec(memory_space=pl.ANY)
VMEM = pl.BlockSpec(memory_space=pltpu.VMEM)


def below_y(field, row):
    y = lax.broadcasted_iota(jnp.int32, field.shape, 0)
    return jnp.where(y == 0, row, pltpu.roll(field, 1, 0))


def above_y(field, row):
    count = field.shape[0]
    y = lax.broadcasted_iota(jnp.int32, field.shape, 0)
    return jnp.where(y == count - 1, row, pltpu.roll(field, count - 1, 0))


def below_z(field):
    z = lax.broadcasted_iota(jnp.int32, field.shape, 1)
    return jnp.where(z == 0, 0.0, pltpu.roll(field, 1, 1))


def above_z(field):
    count = field.shape[1]
    z = lax.broadcasted_iota(jnp.int32, field.shape, 1)
    return jnp.where(z == count - 1, 0.0, pltpu.roll(field, count - 1, 1))


def velocity_plane(vel, scaled, sxx, sxx_next, syy, syy_row, szz, sxy, sxy_prior, sxy_row, sxz, sxz_prior, syz, syz_row):
    vx, vy, vz = vel
    vx = vx - scaled * (sxx_next - sxx + (sxy - below_y(sxy, sxy_row)) + (sxz - below_z(sxz)))
    vy = vy - scaled * (sxy - sxy_prior + (above_y(syy, syy_row) - syy) + (syz - below_z(syz)))
    vz = vz - scaled * (sxz - sxz_prior + (syz - below_y(syz, syz_row)) + (above_z(szz) - szz))
    return vx, vy, vz


def strain_plane(vx, vx_prior, vx_row, vy, vy_next, vy_row, vz, vz_next, vz_row):
    exx = vx - vx_prior
    eyy = vy - below_y(vy, vy_row)
    ezz = vz - below_z(vz)
    exy = (above_y(vx, vx_row) - vx) + (vy_next - vy)
    exz = (above_z(vx) - vx) + (vz_next - vz)
    eyz = (above_z(vy) - vy) + (above_y(vz, vz_row) - vz)
    return exx, eyy, ezz, exy, exz, eyz


def stress_plane(stress, strain, lam, mu):
    trace = strain[0] + strain[1] + strain[2]
    direct = [stress[k] - courant * (lam * trace + 2.0 * mu * strain[k]) for k in range(3)]
    shear = [stress[k] - courant * mu * strain[k] for k in range(3, 6)]
    return direct + shear


UP_PLANES = (6, 7, 11)
DOWN_PLANES = (3, 10, 11)
UP_ROWS = (6, 8, 11, 1, 9, 4)
DOWN_ROWS = (4, 10, 11, 0, 9, 3, 6, 7)


def on_lower_core():
    return lax.axis_index("gx") % 2 == 0


def below_above(far, near):
    lower = on_lower_core()
    return lambda k: jnp.where(lower, far[k], near[k]), lambda k: jnp.where(lower, near[k], far[k])


def far_near(up, down):
    lower = on_lower_core()
    return jnp.where(lower, down, up), jnp.where(lower, up, down)


def prepare(adj, buoy, lam, mu, far, near, to_next_y, to_prior_y, rows, sems, row_sems):
    cells_x, cells_y = adj.shape[1:3]
    extra = (buoy, lam, mu)

    def whole(n):
        return adj.at[n] if n < 9 else extra[n - 9]

    def planes(core):
        plans = []
        for target, names, x in ((far, DOWN_PLANES, 0), (near, UP_PLANES, cells_x - 1)) if core == 0 else ((far, UP_PLANES, cells_x - 1), (near, DOWN_PLANES, 0)):
            plans += [(whole(n).at[x], target.at[k]) for k, n in enumerate(names)]
        return [pltpu.make_async_copy(source, target, sems.at[k]) for k, (source, target) in enumerate(plans)]

    def both(verb):
        lower = on_lower_core()
        for core in range(2):

            @pl.when(lower == (core == 0))
            def _():
                for copy in planes(core):
                    getattr(copy, verb)()

    both("start")
    plans = [(n, cells_y - 8) for n in UP_ROWS] + [(n, 0) for n in DOWN_ROWS]
    copies = [
        pltpu.make_async_copy(whole(n).at[:, pl.ds(start, 8)], rows.at[k], row_sems.at[k]) for k, (n, start) in enumerate(plans)
    ]
    for copy in copies:
        copy.start()
    for copy in copies:
        copy.wait()
    for k in range(len(UP_ROWS)):
        to_next_y[k] = rows[k, :, 7, :]
    for k in range(len(DOWN_ROWS)):
        to_prior_y[k] = rows[len(UP_ROWS) + k, :, 0, :]
    both("wait")


def merge(packed, scales, message):
    comp, _, count = scales.shape
    per = packed.shape[0] // count
    factor = jnp.pad(scales[:, 0, :], ((0, 128 - comp), (0, 128 - count)))
    factor = (jnp.transpose(factor)[:count] * FACTOR_UP).astype(jnp.int32)
    message[pl.ds(per, count, stride=per + 1), :] = factor
    for r in range(per):
        message[pl.ds(r, count, stride=per + 1), :] = packed[pl.ds(r, count, stride=per), :]


def first_velocity(adj, buoy, far_in, near_in, prior_y, next_y, v, far, near, to_next_y, to_prior_y):
    cells_x, cells_y = adj.shape[1:3]
    last = cells_x - 1
    below, above = below_above(far_in, near_in)
    for x in range(cells_x):
        new = velocity_plane(
            (adj[0, x], adj[1, x], adj[2, x]), courant * buoy[x],
            adj[3, x], adj[3, x + 1] if x < last else above(0), adj[4, x], next_y[0, x : x + 1], adj[5, x],
            adj[6, x], adj[6, x - 1] if x > 0 else below(0), prior_y[0, x : x + 1],
            adj[7, x], adj[7, x - 1] if x > 0 else below(1), adj[8, x], prior_y[1, x : x + 1],
        )
        for k in range(3):
            v[k, x] = new[k]
            to_next_y[k, x : x + 1, :] = new[k][cells_y - 1 :, :]
            to_prior_y[k, x : x + 1, :] = new[k][0:1, :]
    own = {n: next_y[k, last : last + 1] for k, n in enumerate(DOWN_ROWS)}
    scaled_up = courant * own[9]
    sides = (own[6] - adj[6, last][cells_y - 1 :, :]) + (own[7] - below_z(own[7]))
    part_up = own[0] - scaled_up * (sides - own[3])
    own = {n: prior_y[k, 0:1] for k, n in enumerate(UP_ROWS)}
    scaled_down = courant * own[9]
    sides = (adj[4, 0][0:1, :] - own[4]) + (own[8] - below_z(own[8]))
    part_down = own[1] - scaled_down * (own[6] + sides)
    for k in range(3):
        far[pl.ds(k * cells_y, cells_y), :], near[pl.ds(k * cells_y, cells_y), :] = far_near(v[k, last], v[k, 0])
    at = 3 * cells_y
    far[at : at + 1, :], near[at : at + 1, :] = far_near(part_up, part_down)
    far[at + 1 : at + 2, :], near[at + 1 : at + 2, :] = far_near(scaled_up, scaled_down)


def middle(
    adj, buoy, lam, mu, s_far, s_near, s_prior_y, s_next_y, v, last_y, first_y, v_far, v_near, v_prior_y, v_next_y,
    v_new, stress, strain, far, near, to_next_y, to_prior_y,
):
    cells_x, cells_y = adj.shape[1:3]
    last = cells_x - 1
    s_below, s_above = below_above(s_far, s_near)
    v_below, v_above = below_above(v_far, v_near)
    vx_m, vy_m, vz_m = (v_below(pl.ds(k * cells_y, cells_y)) for k in range(3))
    vx_n, vy_n, vz_n = (v_above(pl.ds(k * cells_y, cells_y)) for k in range(3))
    part, scaled = pl.ds(3 * cells_y, 1), pl.ds(3 * cells_y + 1, 1)
    vx_corner = v_below(part) - v_below(scaled) * s_next_y[DOWN_ROWS.index(3), 0:1]
    vy_corner = v_above(part) + v_above(scaled) * s_prior_y[UP_ROWS.index(6), last : last + 1]
    exx = vx_n - v[0, last]
    trace = exx + (vy_n - below_y(vy_n, vy_corner)) + (vz_n - below_z(vz_n))
    sxx_next = s_above(0) - courant * (s_above(1) * trace + 2.0 * s_above(2) * exx)
    exy = (above_y(vx_m, vx_corner) - vx_m) + (v[1, 0] - vy_m)
    exz = (above_z(vx_m) - vx_m) + (v[2, 0] - vz_m)
    sxy_prior = s_below(0) - courant * s_below(2) * exy
    sxz_prior = s_below(1) - courant * s_below(2) * exz
    over = v_next_y[0]
    exx = over - jnp.concatenate([vx_corner, over[:last]], axis=0)
    eyy = v_next_y[1] - last_y[1]
    trace = exx + eyy + (v_next_y[2] - below_z(v_next_y[2]))
    syy_rows = s_next_y[0] - courant * (s_next_y[1] * trace + 2.0 * s_next_y[2] * eyy)
    under = v_prior_y[1]
    exy = (first_y[0] - v_prior_y[0]) + (jnp.concatenate([under[1:], vy_corner], axis=0) - under)
    eyz = (above_z(under) - under) + (first_y[2] - v_prior_y[2])
    sxy_rows = s_prior_y[0] - courant * s_prior_y[2] * exy
    syz_rows = s_prior_y[1] - courant * s_prior_y[2] * eyz
    for x in range(cells_x):
        e = strain_plane(
            v[0, x], v[0, x - 1] if x > 0 else vx_m, v_next_y[0, x : x + 1],
            v[1, x], v[1, x + 1] if x < last else vy_n, v_prior_y[1, x : x + 1],
            v[2, x], v[2, x + 1] if x < last else vz_n, v_next_y[2, x : x + 1],
        )
        s = stress_plane([adj[3 + k, x] for k in range(6)], e, lam[x], mu[x])
        for k in range(6):
            strain[k, x] = e[k]
            stress[k, x] = s[k]
    for x in range(cells_x):
        new = velocity_plane(
            (v[0, x], v[1, x], v[2, x]), courant * buoy[x],
            stress[0, x], stress[0, x + 1] if x < last else sxx_next, stress[1, x], syy_rows[x : x + 1], stress[2, x],
            stress[3, x], stress[3, x - 1] if x > 0 else sxy_prior, sxy_rows[x : x + 1],
            stress[4, x], stress[4, x - 1] if x > 0 else sxz_prior, stress[5, x], syz_rows[x : x + 1],
        )
        for k in range(3):
            v_new[k, x] = new[k]
        to_next_y[0, x : x + 1, :] = new[1][cells_y - 1 :, :]
        to_prior_y[0, x : x + 1, :] = new[0][0:1, :]
        to_prior_y[1, x : x + 1, :] = new[2][0:1, :]
    far[0], near[0] = far_near(v_new[0, last], v_new[1, 0])
    far[1], near[1] = far_near(jnp.zeros_like(v_new[2, 0]), v_new[2, 0])


def second_stress(v, stress, lam, mu, v_far, v_near, prior_y, next_y, out, strain):
    cells_x = v.shape[1]
    last = cells_x - 1
    below, above = below_above(v_far, v_near)
    for x in range(cells_x):
        e = strain_plane(
            v[0, x], v[0, x - 1] if x > 0 else below(0), next_y[0, x : x + 1],
            v[1, x], v[1, x + 1] if x < last else above(0), prior_y[0, x : x + 1],
            v[2, x], v[2, x + 1] if x < last else above(1), next_y[1, x : x + 1],
        )
        s = stress_plane([stress[k, x] for k in range(6)], e, lam[x], mu[x])
        for k in range(3):
            out[k, x] = v[k, x]
        for k in range(6):
            strain[k, x] = e[k]
            out[3 + k, x] = s[k]


def gradients(message, perm, strain1, strain2, out):
    count = perm.shape[1]
    per = message.shape[0] // count
    cells_x, cells_y, cells_z = strain1.shape[1:]
    rows = cells_x * cells_y
    both = jnp.concatenate([perm[...], perm[...]], axis=1)
    r = lax.broadcasted_iota(jnp.int32, (rows, 2 * count), 0)
    k = lax.broadcasted_iota(jnp.int32, (rows, 2 * count), 1)
    mine = both == lax.shift_right_logical(r, 1)
    half = (k >= count) == ((r & 1) == 1)
    pick = jnp.where(mine & half, 1.0, 0.0).astype(jnp.bfloat16)
    pick_factor = jnp.where(mine & (k < count), 1.0, 0.0)
    factor = message[pl.ds(per - 1, count, stride=per), :].astype(F32) * FACTOR_DOWN
    factor = jnp.concatenate([factor, jnp.zeros_like(factor)], axis=0)
    factor = lax.dot(pick_factor, factor, precision=lax.Precision.HIGHEST, preferred_element_type=F32)

    def forward(c):
        w = [message[pl.ds(2 * c + t, count, stride=per), :] for t in range(2)]
        byte = [lambda w: w & 255, lambda w: lax.shift_right_logical(w, 8) & 255, lambda w: lax.shift_right_logical(w, 16) & 255]
        parts = [[(f(v) - 128) for v in w] for f in byte] + [[lax.shift_right_arithmetic(v, 24) for v in w]]
        parts = [[v.astype(F32).astype(jnp.bfloat16) for v in p] for p in parts]
        low = jnp.concatenate(parts[0] + parts[1], axis=1)
        high = jnp.concatenate(parts[2] + parts[3], axis=1)
        table = jnp.concatenate([low, high], axis=0)
        picked = lax.dot(pick, table, preferred_element_type=F32)
        return picked * factor[:, c : c + 1]

    grad_lambda = None
    grad_mu = None
    for step, strain in enumerate((strain1, strain2)):
        f = [forward(6 * step + n) for n in range(6)]
        e = [strain[n].reshape(rows, cells_z) for n in range(6)]
        add_lambda = (e[0] + e[1] + e[2]) * (f[0] + f[1] + f[2])
        add_mu = 2.0 * (e[0] * f[0] + e[1] * f[1] + e[2] * f[2])
        grad_lambda = add_lambda if step == 0 else grad_lambda + add_lambda
        grad_mu = add_mu if step == 0 else grad_mu + add_mu
        grad_mu = grad_mu + e[3] * f[3] + e[4] * f[4] + e[5] * f[5]
    out[0] = grad_lambda.reshape(cells_x, cells_y, cells_z)
    out[1] = grad_mu.reshape(cells_x, cells_y, cells_z)


def on_device(adjoint, buoyancy, lame_lambda, shear_mu, packed, scales, perm):
    cells_x, cells_y, cells_z = buoyancy.shape
    owners, comp, width = packed.shape[1], packed.shape[3], packed.shape[4]
    per = comp * width // 128

    def shape(*dims, dtype=F32):
        return jax.ShapeDtypeStruct(dims, dtype)

    def call(kernel, mebibytes, outs, args, in_specs=None, scratch=()):
        return pl.pallas_call(
            kernel,
            out_shape=outs,
            in_specs=in_specs or [VMEM] * len(args),
            out_specs=jax.tree.map(lambda _: VMEM, outs),
            scratch_shapes=scratch,
            compiler_params=pltpu.CompilerParams(vmem_limit_bytes=mebibytes << 20),
        )(*args)

    count_x = lax.axis_size("gx")
    count_y = lax.axis_size("gy")
    off_chip = [(x, x + 1 if x % 2 else x - 1) for x in range(1, count_x - 1)]
    on_chip = [(x, x ^ 1) for x in range(count_x)]
    upward = [(y, y + 1) for y in range(count_y - 1)]
    downward = [(y + 1, y) for y in range(count_y - 1)]

    def swap(far, near, to_next_y, to_prior_y):
        far = lax.ppermute(far, "gx", off_chip)
        near = lax.ppermute(near, "gx", on_chip)
        prior_y = lax.ppermute(to_next_y, "gy", upward)
        next_y = lax.ppermute(to_prior_y, "gy", downward)
        return far, near, prior_y, next_y

    def planes(*count):
        return shape(*count, cells_y, cells_z)

    def lines(count):
        return shape(count, cells_x, cells_z)

    sent = call(
        prepare, 8, (planes(3), planes(3), lines(len(UP_ROWS)), lines(len(DOWN_ROWS))),
        (adjoint, buoyancy, lame_lambda, shear_mu), [ANY] * 4,
        [
            pltpu.VMEM((len(UP_ROWS) + len(DOWN_ROWS), cells_x, 8, cells_z), F32),
            pltpu.SemaphoreType.DMA((6,)),
            pltpu.SemaphoreType.DMA((len(UP_ROWS) + len(DOWN_ROWS),)),
        ],
    )
    s_ghosts = swap(*sent)

    by_comp = jnp.transpose(scales.reshape(owners, comp)).reshape(comp, 1, owners)
    message = call(merge, 8, shape(owners * (per + 1), 128, dtype=jnp.int32), (packed.reshape(owners * per, 128), by_comp))
    message = lax.all_to_all(message.reshape(owners, per + 1, 1, 128), "gx", split_axis=0, concat_axis=0, tiled=True)
    message = message.reshape(owners * (per + 1), 128)

    faces = shape(3 * cells_y + 8, cells_z)
    v, *sent = call(
        first_velocity, 12, (planes(3, cells_x), faces, faces, lines(3), lines(3)), (adjoint, buoyancy, *s_ghosts)
    )
    last_y, first_y = sent[2:]
    v_ghosts = swap(*sent)

    v, stress, strain1, *sent = call(
        middle, 16,
        (planes(3, cells_x), planes(6, cells_x), planes(6, cells_x), planes(2), planes(2), lines(1), lines(2)),
        (adjoint, buoyancy, lame_lambda, shear_mu, *s_ghosts, v, last_y, first_y, *v_ghosts),
    )
    v_ghosts = swap(*sent)

    adjoint_out, strain2 = call(
        second_stress, 12, (shape(*adjoint.shape), planes(6, cells_x)), (v, stress, lame_lambda, shear_mu, *v_ghosts)
    )
    grads = call(gradients, 16, planes(2, cells_x), (message, perm, strain1, strain2))
    return adjoint_out, grads


def solution(mesh):
    return jax.shard_map(
        on_device,
        mesh=mesh,
        in_specs=(
            P(None, "gx", "gy", None),
            P("gx", "gy", None),
            P("gx", "gy", None),
            P("gx", "gy", None),
            P("gx", None, "gy", None, None),
            P("gx", None, "gy", None),
            P("gx", None),
        ),
        out_specs=(P(None, "gx", "gy", None), P(None, "gx", "gy", None)),
        check_vma=False,
    )
```

```python
import jax
import jax.numpy as jnp
from jax import lax
from jax.experimental import pallas as pl
from jax.experimental.pallas import tpu as pltpu
from jax.sharding import PartitionSpec as P


courant = 0.15
FACTOR_UP = 2.0**35
FACTOR_DOWN = 2.0**-35
F32 = jnp.float32
ANY = pl.BlockSpec(memory_space=pl.ANY)
VMEM = pl.BlockSpec(memory_space=pltpu.VMEM)


def below_y(field, row):
    y = lax.broadcasted_iota(jnp.int32, field.shape, 0)
    return jnp.where(y == 0, row, pltpu.roll(field, 1, 0))


def above_y(field, row):
    count = field.shape[0]
    y = lax.broadcasted_iota(jnp.int32, field.shape, 0)
    return jnp.where(y == count - 1, row, pltpu.roll(field, count - 1, 0))


def below_z(field):
    z = lax.broadcasted_iota(jnp.int32, field.shape, 1)
    return jnp.where(z == 0, 0.0, pltpu.roll(field, 1, 1))


def above_z(field):
    count = field.shape[1]
    z = lax.broadcasted_iota(jnp.int32, field.shape, 1)
    return jnp.where(z == count - 1, 0.0, pltpu.roll(field, count - 1, 1))


def velocity_plane(vel, scaled, sxx, sxx_next, syy, syy_row, szz, sxy, sxy_prior, sxy_row, sxz, sxz_prior, syz, syz_row):
    vx, vy, vz = vel
    vx = vx - scaled * (sxx_next - sxx + (sxy - below_y(sxy, sxy_row)) + (sxz - below_z(sxz)))
    vy = vy - scaled * (sxy - sxy_prior + (above_y(syy, syy_row) - syy) + (syz - below_z(syz)))
    vz = vz - scaled * (sxz - sxz_prior + (syz - below_y(syz, syz_row)) + (above_z(szz) - szz))
    return vx, vy, vz


def strain_plane(vx, vx_prior, vx_row, vy, vy_next, vy_row, vz, vz_next, vz_row):
    exx = vx - vx_prior
    eyy = vy - below_y(vy, vy_row)
    ezz = vz - below_z(vz)
    exy = (above_y(vx, vx_row) - vx) + (vy_next - vy)
    exz = (above_z(vx) - vx) + (vz_next - vz)
    eyz = (above_z(vy) - vy) + (above_y(vz, vz_row) - vz)
    return exx, eyy, ezz, exy, exz, eyz


def stress_plane(stress, strain, lam, mu):
    trace = strain[0] + strain[1] + strain[2]
    direct = [stress[k] - courant * (lam * trace + 2.0 * mu * strain[k]) for k in range(3)]
    shear = [stress[k] - courant * mu * strain[k] for k in range(3, 6)]
    return direct + shear


UP_PLANES = (6, 7, 11)
DOWN_PLANES = (3, 10, 11)
UP_ROWS = (6, 8, 11, 1, 9, 4)
DOWN_ROWS = (4, 10, 11, 0, 9, 3, 6, 7)


def on_lower_core():
    return lax.axis_index("gx") % 2 == 0


def below_above(far, near):
    lower = on_lower_core()
    return lambda k: jnp.where(lower, far[k], near[k]), lambda k: jnp.where(lower, near[k], far[k])


def far_near(up, down):
    lower = on_lower_core()
    return jnp.where(lower, down, up), jnp.where(lower, up, down)


def on_even_row():
    return lax.axis_index("gy") % 2 == 0


def prior_next(first, second):
    even = on_even_row()
    return jnp.where(even, second[...], first[...]), jnp.where(even, first[...], second[...])


def first_second(to_next, to_prior):
    even = on_even_row()
    return jnp.where(even, to_next, to_prior), jnp.where(even, to_prior, to_next)


def prepare(adj, buoy, lam, mu, far, near, first, second, rows, sems, row_sems):
    cells_x, cells_y = adj.shape[1:3]
    extra = (buoy, lam, mu)

    def whole(n):
        return adj.at[n] if n < 9 else extra[n - 9]

    def planes(core):
        plans = []
        for target, names, x in ((far, DOWN_PLANES, 0), (near, UP_PLANES, cells_x - 1)) if core == 0 else ((far, UP_PLANES, cells_x - 1), (near, DOWN_PLANES, 0)):
            plans += [(whole(n).at[x], target.at[k]) for k, n in enumerate(names)]
        return [pltpu.make_async_copy(source, target, sems.at[k]) for k, (source, target) in enumerate(plans)]

    def both(verb):
        lower = on_lower_core()
        for core in range(2):

            @pl.when(lower == (core == 0))
            def _():
                for copy in planes(core):
                    getattr(copy, verb)()

    both("start")
    plans = [(n, cells_y - 8) for n in UP_ROWS] + [(n, 0) for n in DOWN_ROWS]
    copies = [
        pltpu.make_async_copy(whole(n).at[:, pl.ds(start, 8)], rows.at[k], row_sems.at[k]) for k, (n, start) in enumerate(plans)
    ]
    for copy in copies:
        copy.start()
    for copy in copies:
        copy.wait()
    for k in range(len(DOWN_ROWS)):
        down = rows[len(UP_ROWS) + k, :, 0, :]
        up = rows[k, :, 7, :] if k < len(UP_ROWS) else jnp.zeros_like(down)
        first[k], second[k] = first_second(up, down)
    both("wait")


def merge(packed, scales, message, words, build, word_sems, sems):
    comp, _, count = scales.shape
    per = packed.shape[0] // count
    size = 16
    starts = range(0, count, size)
    loads = []
    for n, start in enumerate(starts):
        part = pl.ds(start * per, size * per)
        loads.append(pltpu.make_async_copy(packed.at[part], words.at[part], word_sems.at[n]))
        loads[-1].start()
    factor = jnp.pad(scales[:, 0, :], ((0, 128 - comp), (0, 128 - count)))
    factor = (jnp.transpose(factor)[:count] * FACTOR_UP).astype(jnp.int32)
    build[pl.ds(per, count, stride=per + 1), :] = factor
    copies = []
    for n, start in enumerate(starts):
        loads[n].wait()
        for r in range(per):
            build[pl.ds(start * (per + 1) + r, size, stride=per + 1), :] = words[pl.ds(start * per + r, size, stride=per), :]
        part = pl.ds(start * (per + 1), size * (per + 1))
        copies.append(pltpu.make_async_copy(build.at[part], message.at[part], sems.at[n]))
        copies[-1].start()
    for copy in copies:
        copy.wait()


def first_velocity(adj, buoy, far_in, near_in, first_in, second_in, v_out, far, near, first, second, v, sems):
    prior_y, next_y = prior_next(first_in, second_in)
    cells_x, cells_y = adj.shape[1:3]
    last = cells_x - 1
    below, above = below_above(far_in, near_in)
    for x in range(cells_x):
        new = velocity_plane(
            (adj[0, x], adj[1, x], adj[2, x]), courant * buoy[x],
            adj[3, x], adj[3, x + 1] if x < last else above(0), adj[4, x], next_y[0, x : x + 1], adj[5, x],
            adj[6, x], adj[6, x - 1] if x > 0 else below(0), prior_y[0, x : x + 1],
            adj[7, x], adj[7, x - 1] if x > 0 else below(1), adj[8, x], prior_y[1, x : x + 1],
        )
        for k in range(3):
            v[k, x] = new[k]
    copy = pltpu.make_async_copy(v, v_out, sems.at[0])
    copy.start()
    for k in range(3):
        first[k], second[k] = first_second(v[k, :, cells_y - 1, :], v[k, :, 0, :])
    own = {n: next_y[k, last : last + 1] for k, n in enumerate(DOWN_ROWS)}
    scaled_up = courant * own[9]
    sides = (own[6] - adj[6, last][cells_y - 1 :, :]) + (own[7] - below_z(own[7]))
    part_up = own[0] - scaled_up * (sides - own[3])
    own = {n: prior_y[k, 0:1] for k, n in enumerate(UP_ROWS)}
    scaled_down = courant * own[9]
    sides = (adj[4, 0][0:1, :] - own[4]) + (own[8] - below_z(own[8]))
    part_down = own[1] - scaled_down * (own[6] + sides)
    for k in range(3):
        far[pl.ds(k * cells_y, cells_y), :], near[pl.ds(k * cells_y, cells_y), :] = far_near(v[k, last], v[k, 0])
    at = 3 * cells_y
    far[at : at + 1, :], near[at : at + 1, :] = far_near(part_up, part_down)
    far[at + 1 : at + 2, :], near[at + 1 : at + 2, :] = far_near(scaled_up, scaled_down)
    copy.wait()


def half(
    adj, buoy, lam, mu, s_far, s_near, s_prior_y, s_next_y, v, v_far, v_near, v_prior_y, v_next_y,
    v_new, stress, strain, between,
):
    cells_x, cells_y = adj.shape[1:3]
    last = cells_x - 1
    s_below, s_above = below_above(s_far, s_near)
    v_below, v_above = below_above(v_far, v_near)
    vx_m, vy_m, vz_m = (v_below(pl.ds(k * cells_y, cells_y)) for k in range(3))
    vx_n, vy_n, vz_n = (v_above(pl.ds(k * cells_y, cells_y)) for k in range(3))
    part, scaled = pl.ds(3 * cells_y, 1), pl.ds(3 * cells_y + 1, 1)
    vx_corner = v_below(part) - v_below(scaled) * s_next_y[DOWN_ROWS.index(3), 0:1]
    vy_corner = v_above(part) + v_above(scaled) * s_prior_y[UP_ROWS.index(6), last : last + 1]
    exx = vx_n - v[0, last]
    trace = exx + (vy_n - below_y(vy_n, vy_corner)) + (vz_n - below_z(vz_n))
    sxx_next = s_above(0) - courant * (s_above(1) * trace + 2.0 * s_above(2) * exx)
    exy = (above_y(vx_m, vx_corner) - vx_m) + (v[1, 0] - vy_m)
    exz = (above_z(vx_m) - vx_m) + (v[2, 0] - vz_m)
    sxy_prior = s_below(0) - courant * s_below(2) * exy
    sxz_prior = s_below(1) - courant * s_below(2) * exz
    over = v_next_y[0]
    exx = over - jnp.concatenate([vx_corner, over[:last]], axis=0)
    eyy = v_next_y[1] - v[1, :, cells_y - 1, :]
    trace = exx + eyy + (v_next_y[2] - below_z(v_next_y[2]))
    syy_rows = s_next_y[0] - courant * (s_next_y[1] * trace + 2.0 * s_next_y[2] * eyy)
    under = v_prior_y[1]
    exy = (v[0, :, 0, :] - v_prior_y[0]) + (jnp.concatenate([under[1:], vy_corner], axis=0) - under)
    eyz = (above_z(under) - under) + (v[2, :, 0, :] - v_prior_y[2])
    sxy_rows = s_prior_y[0] - courant * s_prior_y[2] * exy
    syz_rows = s_prior_y[1] - courant * s_prior_y[2] * eyz
    for x in range(cells_x):
        e = strain_plane(
            v[0, x], v[0, x - 1] if x > 0 else vx_m, v_next_y[0, x : x + 1],
            v[1, x], v[1, x + 1] if x < last else vy_n, v_prior_y[1, x : x + 1],
            v[2, x], v[2, x + 1] if x < last else vz_n, v_next_y[2, x : x + 1],
        )
        s = stress_plane([adj[3 + k, x] for k in range(6)], e, lam[x], mu[x])
        for k in range(6):
            stress[k, x] = s[k]
            if strain is not None:
                strain[k, x] = e[k]
    between()
    for x in range(cells_x):
        new = velocity_plane(
            (v[0, x], v[1, x], v[2, x]), courant * buoy[x],
            stress[0, x], stress[0, x + 1] if x < last else sxx_next, stress[1, x], syy_rows[x : x + 1], stress[2, x],
            stress[3, x], stress[3, x - 1] if x > 0 else sxy_prior, sxy_rows[x : x + 1],
            stress[4, x], stress[4, x - 1] if x > 0 else sxz_prior, stress[5, x], syz_rows[x : x + 1],
        )
        for k in range(3):
            v_new[k, x] = new[k]


def middle(
    adj, buoy, lam_in, mu_in, s_far_in, s_near_in, v_in, s_first, s_second, v_far, v_near, v_first, v_second,
    fields, strain_out, far, near, first, second, lam, mu, s_far, s_near, v, v_new, stress, strain, load_sems, sems,
):
    plans = ((lam_in, lam), (mu_in, mu), (s_far_in, s_far), (s_near_in, s_near), (v_in, v))
    loads = [pltpu.make_async_copy(source, target, load_sems.at[n]) for n, (source, target) in enumerate(plans)]
    for copy in loads:
        copy.start()
    copies = [
        pltpu.make_async_copy(strain, strain_out, sems.at[0]),
        pltpu.make_async_copy(stress, fields.at[pl.ds(3, 6)], sems.at[1]),
        pltpu.make_async_copy(v_new, fields.at[pl.ds(0, 3)], sems.at[2]),
    ]
    for copy in loads:
        copy.wait()
    half(
        adj, buoy, lam, mu, s_far, s_near, *prior_next(s_first, s_second), v, v_far, v_near, *prior_next(v_first, v_second),
        v_new, stress, strain, lambda: [copy.start() for copy in copies[:2]],
    )
    copies[2].start()
    _, cells_x, cells_y, _ = v_new.shape
    over, under = v_new[1, :, cells_y - 1, :], v_new[0, :, 0, :]
    first[0], second[0] = first_second(over, under)
    under = v_new[2, :, 0, :]
    first[1], second[1] = first_second(jnp.zeros_like(under), under)
    far[0], near[0] = far_near(v_new[0, cells_x - 1], v_new[1, 0])
    far[1], near[1] = far_near(jnp.zeros_like(v_new[2, 0]), v_new[2, 0])
    for copy in copies:
        copy.wait()


def finish(
    fields, lam_in, mu_in, strain_in, perm_in, v_far, v_near, v_first, v_second, message, out, out_grads,
    v, stress, lam, mu, strain1, perm, strain2, forward, grads, sems,
):
    plans = ((fields.at[pl.ds(0, 3)], v), (fields.at[pl.ds(3, 6)], stress), (lam_in, lam), (mu_in, mu), (strain_in, strain1), (perm_in, perm))
    prior_y, next_y = prior_next(v_first, v_second)
    copies = [pltpu.make_async_copy(source, target, sems.at[n]) for n, (source, target) in enumerate(plans)]
    for copy in copies:
        copy.start()
    count = perm.shape[1]
    per = message.shape[0] // count
    cells_x, cells_y, cells_z = strain1.shape[1:]
    rows = cells_x * cells_y
    copies[5].wait()
    both = jnp.concatenate([perm[...], perm[...]], axis=1)
    r = lax.broadcasted_iota(jnp.int32, (rows, 2 * count), 0)
    k = lax.broadcasted_iota(jnp.int32, (rows, 2 * count), 1)
    mine = both == lax.shift_right_logical(r, 1)
    half = (k >= count) == ((r & 1) == 1)
    pick = jnp.where(mine & half, 1.0, 0.0).astype(jnp.bfloat16)
    pick_factor = jnp.where(mine & (k < count), 1.0, 0.0)
    factor = message[pl.ds(per - 1, count, stride=per), :].astype(F32) * FACTOR_DOWN
    factor = jnp.concatenate([factor, jnp.zeros_like(factor)], axis=0)
    factor = lax.dot(pick_factor, factor, precision=lax.Precision.HIGHEST, preferred_element_type=F32)

    for c in range(forward.shape[0]):
        w = [message[pl.ds(2 * c + t, count, stride=per), :] for t in range(2)]
        byte = [lambda w: w & 255, lambda w: lax.shift_right_logical(w, 8) & 255, lambda w: lax.shift_right_logical(w, 16) & 255]
        parts = [[(f(v) - 128) for v in w] for f in byte] + [[lax.shift_right_arithmetic(v, 24) for v in w]]
        parts = [[v.astype(F32).astype(jnp.bfloat16) for v in p] for p in parts]
        low = jnp.concatenate(parts[0] + parts[1], axis=1)
        high = jnp.concatenate(parts[2] + parts[3], axis=1)
        table = jnp.concatenate([low, high], axis=0)
        picked = lax.dot(pick, table, preferred_element_type=F32)
        forward[c] = picked * factor[:, c : c + 1]
    last = cells_x - 1
    below, above = below_above(v_far, v_near)
    for copy in copies[:4]:
        copy.wait()
    for x in range(cells_x):
        e = strain_plane(
            v[0, x], v[0, x - 1] if x > 0 else below(0), next_y[0, x : x + 1],
            v[1, x], v[1, x + 1] if x < last else above(0), prior_y[0, x : x + 1],
            v[2, x], v[2, x + 1] if x < last else above(1), next_y[1, x : x + 1],
        )
        s = stress_plane([stress[k, x] for k in range(6)], e, lam[x], mu[x])
        for k in range(6):
            strain2[k, x] = e[k]
            stress[k, x] = s[k]
    stress_copy = pltpu.make_async_copy(stress, out.at[pl.ds(3, 6)], sems.at[5])
    stress_copy.start()
    copies[4].wait()
    for step, strain in enumerate((strain1, strain2)):
        f = [forward[6 * step + n] for n in range(6)]
        e = [strain[n].reshape(rows, cells_z) for n in range(6)]
        add_lambda = (e[0] + e[1] + e[2]) * (f[0] + f[1] + f[2])
        add_mu = 2.0 * (e[0] * f[0] + e[1] * f[1] + e[2] * f[2])
        grad_lambda = add_lambda if step == 0 else grad_lambda + add_lambda
        grad_mu = add_mu if step == 0 else grad_mu + add_mu
        grad_mu = grad_mu + e[3] * f[3] + e[4] * f[4] + e[5] * f[5]
    grads[0] = grad_lambda.reshape(cells_x, cells_y, cells_z)
    grads[1] = grad_mu.reshape(cells_x, cells_y, cells_z)
    grads_copy = pltpu.make_async_copy(grads, out_grads, sems.at[6])
    grads_copy.start()
    for copy in (stress_copy, grads_copy):
        copy.wait()


def on_device(adjoint, buoyancy, lame_lambda, shear_mu, packed, scales, perm):
    cells_x, cells_y, cells_z = buoyancy.shape
    owners, comp, width = packed.shape[1], packed.shape[3], packed.shape[4]
    per = comp * width // 128

    def shape(*dims, dtype=F32):
        return jax.ShapeDtypeStruct(dims, dtype)

    def in_hbm(*values):
        return [pltpu.with_memory_space_constraint(value, pltpu.HBM) for value in values]

    def call(kernel, mebibytes, outs, args, in_specs=None, scratch=(), out_specs=None, aliases={}):
        return pl.pallas_call(
            kernel,
            out_shape=outs,
            in_specs=in_specs or [VMEM] * len(args),
            out_specs=out_specs or (VMEM,) * len(outs),
            scratch_shapes=scratch,
            compiler_params=pltpu.CompilerParams(vmem_limit_bytes=mebibytes << 20),
            input_output_aliases=aliases,
        )(*args)

    count_x = lax.axis_size("gx")
    count_y = lax.axis_size("gy")
    off_chip = [(x, x + 1 if x % 2 else x - 1) for x in range(1, count_x - 1)]
    on_chip = [(x, x ^ 1) for x in range(count_x)]
    pairs = [[(y, y + 1) for y in range(start, count_y - 1, 2)] for start in (0, 1)]
    pairs = [[*there, *((b, a) for a, b in there)] for there in pairs]

    def swap(far, near, first, second):
        far = lax.ppermute(far, "gx", off_chip)
        near = lax.ppermute(near, "gx", on_chip)
        first = lax.ppermute(first, "gy", pairs[0])
        second = lax.ppermute(second, "gy", pairs[1])
        return far, near, first, second

    def planes(*count):
        return shape(*count, cells_y, cells_z)

    def lines(count):
        return shape(count, cells_x, cells_z)

    sent = call(
        prepare, 8, (planes(3), planes(3), lines(len(DOWN_ROWS)), lines(len(DOWN_ROWS))),
        in_hbm(adjoint, buoyancy, lame_lambda, shear_mu), [ANY] * 4,
        [
            pltpu.VMEM((len(UP_ROWS) + len(DOWN_ROWS), cells_x, 8, cells_z), F32),
            pltpu.SemaphoreType.DMA((6,)),
            pltpu.SemaphoreType.DMA((len(UP_ROWS) + len(DOWN_ROWS),)),
        ],
    )
    s_ghosts = swap(*sent)

    by_comp = jnp.transpose(scales.reshape(owners, comp)).reshape(comp, 1, owners)
    size = (owners * (per + 1), 128)
    (message,) = call(
        merge, 8, (pltpu.HBM(size, jnp.int32),), (*in_hbm(packed.reshape(owners * per, 128)), by_comp), [ANY, VMEM],
        [
            pltpu.VMEM((owners * per, 128), jnp.int32), pltpu.VMEM(size, jnp.int32),
            pltpu.SemaphoreType.DMA((4,)), pltpu.SemaphoreType.DMA((4,)),
        ],
        (ANY,),
    )
    message = lax.all_to_all(message.reshape(owners, per + 1, 1, 128), "gx", split_axis=0, concat_axis=0, tiled=True)
    message = message.reshape(owners * (per + 1), 128)

    faces = shape(3 * cells_y + 8, cells_z)
    strain = (6, cells_x, cells_y, cells_z)
    speeds = (3, cells_x, cells_y, cells_z)
    v, *sent = call(
        first_velocity, 12, (pltpu.HBM(speeds, F32), faces, faces, lines(3), lines(3)), (adjoint, buoyancy, *s_ghosts),
        scratch=[pltpu.VMEM(speeds, F32), pltpu.SemaphoreType.DMA((1,))], out_specs=(ANY, VMEM, VMEM, VMEM, VMEM),
    )
    v_ghosts = swap(*sent)

    fields, strain1, *sent = call(
        middle, 16,
        (pltpu.HBM(adjoint.shape, F32), pltpu.HBM(strain, F32), planes(2), planes(2), lines(2), lines(2)),
        (adjoint, buoyancy, *in_hbm(lame_lambda, shear_mu, *s_ghosts[:2], v), *s_ghosts[2:], *v_ghosts),
        [VMEM] * 2 + [ANY] * 5 + [VMEM] * 6,
        [pltpu.VMEM(size, F32) for size in (speeds[1:], speeds[1:], speeds[:1] + speeds[2:], speeds[:1] + speeds[2:])]
        + [pltpu.VMEM(size, F32) for size in (speeds, speeds, strain, strain)]
        + [pltpu.SemaphoreType.DMA((5,)), pltpu.SemaphoreType.DMA((3,))],
        (ANY, ANY, VMEM, VMEM, VMEM, VMEM),
    )
    v_ghosts = swap(*sent)

    grads = (2, cells_x, cells_y, cells_z)
    adjoint_out, grads = call(
        finish, 24, (pltpu.HBM(adjoint.shape, F32), pltpu.HBM(grads, F32)),
        (*in_hbm(fields, lame_lambda, shear_mu, strain1, perm), *v_ghosts, message),
        [ANY] * 5 + [VMEM] * 5,
        [pltpu.VMEM(size, F32) for size in (speeds, strain, speeds[1:], speeds[1:], strain)]
        + [pltpu.VMEM(perm.shape, jnp.int32)]
        + [pltpu.VMEM(size, F32) for size in (strain, (comp, cells_x * cells_y, cells_z), grads)]
        + [pltpu.SemaphoreType.DMA((7,))],
        (ANY, ANY),
        {0: 0},
    )
    return adjoint_out, grads


def solution(mesh):
    return jax.shard_map(
        on_device,
        mesh=mesh,
        in_specs=(
            P(None, "gx", "gy", None),
            P("gx", "gy", None),
            P("gx", "gy", None),
            P("gx", "gy", None),
            P("gx", None, "gy", None, None),
            P("gx", None, "gy", None),
            P("gx", None),
        ),
        out_specs=(P(None, "gx", "gy", None), P(None, "gx", "gy", None)),
        check_vma=False,
    )
```

```python
import jax
import jax.numpy as jnp
from jax import lax
from jax.experimental import pallas as pl
from jax.experimental.pallas import tpu as pltpu
from jax.sharding import PartitionSpec as P


courant = 0.15
FACTOR_UP = 2.0**35
FACTOR_DOWN = 2.0**-35
F32 = jnp.float32
ANY = pl.BlockSpec(memory_space=pl.ANY)
VMEM = pl.BlockSpec(memory_space=pltpu.VMEM)


def below_y(field, row):
    y = lax.broadcasted_iota(jnp.int32, field.shape, 0)
    return jnp.where(y == 0, row, pltpu.roll(field, 1, 0))


def above_y(field, row):
    count = field.shape[0]
    y = lax.broadcasted_iota(jnp.int32, field.shape, 0)
    return jnp.where(y == count - 1, row, pltpu.roll(field, count - 1, 0))


def below_z(field):
    z = lax.broadcasted_iota(jnp.int32, field.shape, 1)
    return jnp.where(z == 0, 0.0, pltpu.roll(field, 1, 1))


def above_z(field):
    count = field.shape[1]
    z = lax.broadcasted_iota(jnp.int32, field.shape, 1)
    return jnp.where(z == count - 1, 0.0, pltpu.roll(field, count - 1, 1))


def velocity_plane(vel, scaled, sxx, sxx_next, syy, syy_row, szz, sxy, sxy_prior, sxy_row, sxz, sxz_prior, syz, syz_row):
    vx, vy, vz = vel
    vx = vx - scaled * (sxx_next - sxx + (sxy - below_y(sxy, sxy_row)) + (sxz - below_z(sxz)))
    vy = vy - scaled * (sxy - sxy_prior + (above_y(syy, syy_row) - syy) + (syz - below_z(syz)))
    vz = vz - scaled * (sxz - sxz_prior + (syz - below_y(syz, syz_row)) + (above_z(szz) - szz))
    return vx, vy, vz


def strain_plane(vx, vx_prior, vx_row, vy, vy_next, vy_row, vz, vz_next, vz_row):
    exx = vx - vx_prior
    eyy = vy - below_y(vy, vy_row)
    ezz = vz - below_z(vz)
    exy = (above_y(vx, vx_row) - vx) + (vy_next - vy)
    exz = (above_z(vx) - vx) + (vz_next - vz)
    eyz = (above_z(vy) - vy) + (above_y(vz, vz_row) - vz)
    return exx, eyy, ezz, exy, exz, eyz


def stress_plane(stress, strain, lam, mu):
    trace = strain[0] + strain[1] + strain[2]
    direct = [stress[k] - courant * (lam * trace + 2.0 * mu * strain[k]) for k in range(3)]
    shear = [stress[k] - courant * mu * strain[k] for k in range(3, 6)]
    return direct + shear


UP_PLANES = (6, 7)
DOWN_PLANES = (3,)
UP_ROWS = (6, 8, 11, 1, 9, 4)
DOWN_ROWS = (4, 10, 11, 0, 9, 3, 6, 7)


def on_lower_core():
    return lax.axis_index("gx") % 2 == 0


def below_above(far, near):
    lower = on_lower_core()
    return lambda k: jnp.where(lower, far[k], near[k]), lambda k: jnp.where(lower, near[k], far[k])


def far_near(up, down):
    lower = on_lower_core()
    return jnp.where(lower, down, up), jnp.where(lower, up, down)


def on_even_row():
    return lax.axis_index("gy") % 2 == 0


def prior_next(first, second):
    even = on_even_row()
    return jnp.where(even, second[...], first[...]), jnp.where(even, first[...], second[...])


def first_second(to_next, to_prior):
    even = on_even_row()
    return jnp.where(even, to_next, to_prior), jnp.where(even, to_prior, to_next)


def prepare(adj, buoy, lam, mu, far, near, first, second, rows, sems, row_sems):
    cells_x, cells_y = adj.shape[1:3]
    extra = (buoy, lam, mu)

    def whole(n):
        return adj.at[n] if n < 9 else extra[n - 9]

    def planes(core):
        plans = []
        for target, names, x in ((far, DOWN_PLANES, 0), (near, UP_PLANES, cells_x - 1)) if core == 0 else ((far, UP_PLANES, cells_x - 1), (near, DOWN_PLANES, 0)):
            plans += [(whole(n).at[x], target.at[k]) for k, n in enumerate(names)]
        return [pltpu.make_async_copy(source, target, sems.at[k]) for k, (source, target) in enumerate(plans)]

    def both(verb):
        lower = on_lower_core()
        for core in range(2):

            @pl.when(lower == (core == 0))
            def _():
                for copy in planes(core):
                    getattr(copy, verb)()

    both("start")
    plans = [(n, cells_y - 8) for n in UP_ROWS] + [(n, 0) for n in DOWN_ROWS]
    copies = [
        pltpu.make_async_copy(whole(n).at[:, pl.ds(start, 8)], rows.at[k], row_sems.at[k]) for k, (n, start) in enumerate(plans)
    ]
    for copy in copies:
        copy.start()
    for copy in copies:
        copy.wait()
    for k in range(len(DOWN_ROWS)):
        down = rows[len(UP_ROWS) + k, :, 0, :]
        up = rows[k, :, 7, :] if k < len(UP_ROWS) else jnp.zeros_like(down)
        first[k], second[k] = first_second(up, down)
    both("wait")


def merge(packed, scales, message, words, build, word_sems, sems):
    comp, _, count = scales.shape
    per = packed.shape[0] // count
    size = 16
    starts = range(0, count, size)
    loads = []
    for n, start in enumerate(starts):
        part = pl.ds(start * per, size * per)
        loads.append(pltpu.make_async_copy(packed.at[part], words.at[part], word_sems.at[n]))
        loads[-1].start()
    factor = jnp.pad(scales[:, 0, :], ((0, 128 - comp), (0, 128 - count)))
    factor = (jnp.transpose(factor)[:count] * FACTOR_UP).astype(jnp.int32)
    build[pl.ds(per, count, stride=per + 1), :] = factor
    copies = []
    for n, start in enumerate(starts):
        loads[n].wait()
        for r in range(per):
            build[pl.ds(start * (per + 1) + r, size, stride=per + 1), :] = words[pl.ds(start * per + r, size, stride=per), :]
        part = pl.ds(start * (per + 1), size * (per + 1))
        copies.append(pltpu.make_async_copy(build.at[part], message.at[part], sems.at[n]))
        copies[-1].start()
    for copy in copies:
        copy.wait()


def step_one(adj, buoy, below, above, prior_y, next_y, v):
    cells_x = adj.shape[1]
    last = cells_x - 1
    for x in range(cells_x):
        new = velocity_plane(
            (adj[0, x], adj[1, x], adj[2, x]), courant * buoy[x],
            adj[3, x], adj[3, x + 1] if x < last else above(0), adj[4, x], next_y[0, x : x + 1], adj[5, x],
            adj[6, x], adj[6, x - 1] if x > 0 else below(0), prior_y[0, x : x + 1],
            adj[7, x], adj[7, x - 1] if x > 0 else below(1), adj[8, x], prior_y[1, x : x + 1],
        )
        for k in range(3):
            v[k, x] = new[k]


def faces_of(cells_y):
    return [pl.ds(k * cells_y, cells_y) for k in range(3)], 3 * cells_y, [pl.ds(3 * cells_y + 8 + k * cells_y, cells_y) for k in range(2)]


def first_velocity(adj, buoy, lam, mu, far_in, near_in, first_in, second_in, far, near, first, second, v, planes, sems):
    cells_x, cells_y = adj.shape[1:3]
    last = cells_x - 1
    loads = [
        pltpu.make_async_copy(source, planes.at[k], sems.at[k]) for k, source in enumerate((mu.at[last], lam.at[0], mu.at[0]))
    ]
    for copy in loads:
        copy.start()
    prior_y, next_y = prior_next(first_in, second_in)
    step_one(adj, buoy, *below_above(far_in, near_in), prior_y, next_y, v)
    for k in range(3):
        first[k], second[k] = first_second(v[k, :, cells_y - 1, :], v[k, :, 0, :])
    own = {n: next_y[k, last : last + 1] for k, n in enumerate(DOWN_ROWS)}
    scaled_up = courant * own[9]
    sides = (own[6] - adj[6, last][cells_y - 1 :, :]) + (own[7] - below_z(own[7]))
    part_up = own[0] - scaled_up * (sides - own[3])
    own = {n: prior_y[k, 0:1] for k, n in enumerate(UP_ROWS)}
    scaled_down = courant * own[9]
    sides = (adj[4, 0][0:1, :] - own[4]) + (own[8] - below_z(own[8]))
    part_down = own[1] - scaled_down * (own[6] + sides)
    places, at, others = faces_of(cells_y)
    for k, place in enumerate(places):
        far[place, :], near[place, :] = far_near(v[k, last], v[k, 0])
    far[at : at + 1, :], near[at : at + 1, :] = far_near(part_up, part_down)
    far[at + 1 : at + 2, :], near[at + 1 : at + 2, :] = far_near(scaled_up, scaled_down)
    for copy in loads:
        copy.wait()
    far[others[0], :], near[others[0], :] = far_near(planes[0], planes[1])
    far[others[1], :], near[others[1], :] = far_near(jnp.zeros_like(planes[2]), planes[2])


def half(adj, buoy, lam, mu, s_far, s_near, s_first, s_second, v_far, v_near, v_first, v_second, v, stress, strain, between):
    cells_x, cells_y = adj.shape[1:3]
    last = cells_x - 1
    s_below, s_above = below_above(s_far, s_near)
    v_below, v_above = below_above(v_far, v_near)
    s_prior_y, s_next_y = prior_next(s_first, s_second)
    v_prior_y, v_next_y = prior_next(v_first, v_second)
    step_one(adj, buoy, s_below, s_above, s_prior_y, s_next_y, v)
    places, at, others = faces_of(cells_y)
    vx_m, vy_m, vz_m = (v_below(place) for place in places)
    vx_n, vy_n, vz_n = (v_above(place) for place in places)
    part, scaled = pl.ds(at, 1), pl.ds(at + 1, 1)
    mu_prior, lam_next, mu_next = v_below(others[0]), v_above(others[0]), v_above(others[1])
    vx_corner = v_below(part) - v_below(scaled) * s_next_y[DOWN_ROWS.index(3), 0:1]
    vy_corner = v_above(part) + v_above(scaled) * s_prior_y[UP_ROWS.index(6), last : last + 1]
    exx = vx_n - v[0, last]
    trace = exx + (vy_n - below_y(vy_n, vy_corner)) + (vz_n - below_z(vz_n))
    sxx_next = s_above(0) - courant * (lam_next * trace + 2.0 * mu_next * exx)
    exy = (above_y(vx_m, vx_corner) - vx_m) + (v[1, 0] - vy_m)
    exz = (above_z(vx_m) - vx_m) + (v[2, 0] - vz_m)
    sxy_prior = s_below(0) - courant * mu_prior * exy
    sxz_prior = s_below(1) - courant * mu_prior * exz
    over = v_next_y[0]
    exx = over - jnp.concatenate([vx_corner, over[:last]], axis=0)
    eyy = v_next_y[1] - v[1, :, cells_y - 1, :]
    trace = exx + eyy + (v_next_y[2] - below_z(v_next_y[2]))
    syy_rows = s_next_y[0] - courant * (s_next_y[1] * trace + 2.0 * s_next_y[2] * eyy)
    under = v_prior_y[1]
    exy = (v[0, :, 0, :] - v_prior_y[0]) + (jnp.concatenate([under[1:], vy_corner], axis=0) - under)
    eyz = (above_z(under) - under) + (v[2, :, 0, :] - v_prior_y[2])
    sxy_rows = s_prior_y[0] - courant * s_prior_y[2] * exy
    syz_rows = s_prior_y[1] - courant * s_prior_y[2] * eyz
    for x in range(cells_x):
        e = strain_plane(
            v[0, x], v[0, x - 1] if x > 0 else vx_m, v_next_y[0, x : x + 1],
            v[1, x], v[1, x + 1] if x < last else vy_n, v_prior_y[1, x : x + 1],
            v[2, x], v[2, x + 1] if x < last else vz_n, v_next_y[2, x : x + 1],
        )
        s = stress_plane([adj[3 + k, x] for k in range(6)], e, lam[x], mu[x])
        for k in range(6):
            stress[k, x] = s[k]
            if strain is not None:
                strain[k, x] = e[k]
    between()
    for x in range(cells_x):
        new = velocity_plane(
            (v[0, x], v[1, x], v[2, x]), courant * buoy[x],
            stress[0, x], stress[0, x + 1] if x < last else sxx_next, stress[1, x], syy_rows[x : x + 1], stress[2, x],
            stress[3, x], stress[3, x - 1] if x > 0 else sxy_prior, sxy_rows[x : x + 1],
            stress[4, x], stress[4, x - 1] if x > 0 else sxz_prior, stress[5, x], syz_rows[x : x + 1],
        )
        for k in range(3):
            v[k, x] = new[k]


def load(plans, sems):
    copies = [pltpu.make_async_copy(source, target, sems.at[n]) for n, (source, target) in enumerate(plans)]
    for copy in copies:
        copy.start()
    return copies


def edges(
    adj_in, buoy_in, lam_in, mu_in, s_far_in, s_near_in, s_first_in, s_second_in, v_far, v_near, v_first, v_second,
    far, near, first, second, adj, buoy, lam, mu, s_far, s_near, s_first, s_second, v, stress, sems,
):
    given = (adj_in, buoy_in, lam_in, mu_in, s_far_in, s_near_in, s_first_in, s_second_in)
    here = (adj, buoy, lam, mu, s_far, s_near, s_first, s_second)
    for copy in load(zip(given, here), sems):
        copy.wait()
    half(*here, v_far, v_near, v_first, v_second, v, stress, None, lambda: None)
    _, cells_x, cells_y, _ = v.shape
    over, under = v[1, :, cells_y - 1, :], v[0, :, 0, :]
    first[0], second[0] = first_second(over, under)
    under = v[2, :, 0, :]
    first[1], second[1] = first_second(jnp.zeros_like(under), under)
    far[0], near[0] = far_near(v[0, cells_x - 1], v[1, 0])
    far[1], near[1] = far_near(jnp.zeros_like(v[2, 0]), v[2, 0])


def inner(
    adj_in, buoy_in, lam_in, mu_in, s_far_in, s_near_in, s_first_in, s_second_in, v_far, v_near, v_first, v_second, fields, strain_out,
    adj, buoy, lam, mu, s_far, s_near, s_first, s_second, v, stress, strain, load_sems, sems,
):
    given = (adj_in, buoy_in, lam_in, mu_in, s_far_in, s_near_in, s_first_in, s_second_in)
    here = (adj, buoy, lam, mu, s_far, s_near, s_first, s_second)
    for copy in load(zip(given, here), load_sems):
        copy.wait()
    copies = [
        pltpu.make_async_copy(strain, strain_out, sems.at[0]),
        pltpu.make_async_copy(stress, fields.at[pl.ds(3, 6)], sems.at[1]),
        pltpu.make_async_copy(v, fields.at[pl.ds(0, 3)], sems.at[2]),
    ]
    half(*here, v_far, v_near, v_first, v_second, v, stress, strain, lambda: [copy.start() for copy in copies[:2]])
    copies[2].start()
    for copy in copies:
        copy.wait()


def finish(
    fields, lam_in, mu_in, strain_in, perm_in, far, near, first, second, message, out, out_grads,
    v, stress, lam, mu, strain1, perm, strain2, forward, grads, load_sems, sems,
):
    cells_x, cells_y, cells_z = strain1.shape[1:]
    plans = (
        (fields.at[pl.ds(0, 3)], v), (perm_in, perm), (fields.at[pl.ds(3, 6)], stress), (lam_in, lam), (mu_in, mu), (strain_in, strain1),
    )
    copies = load(plans, load_sems)
    count = perm.shape[1]
    per = message.shape[0] // count
    rows = cells_x * cells_y
    copies[1].wait()
    both = jnp.concatenate([perm[...], perm[...]], axis=1)
    r = lax.broadcasted_iota(jnp.int32, (rows, 2 * count), 0)
    k = lax.broadcasted_iota(jnp.int32, (rows, 2 * count), 1)
    mine = both == lax.shift_right_logical(r, 1)
    half = (k >= count) == ((r & 1) == 1)
    pick = jnp.where(mine & half, 1.0, 0.0).astype(jnp.bfloat16)
    pick_factor = jnp.where(mine & (k < count), 1.0, 0.0)
    factor = message[pl.ds(per - 1, count, stride=per), :].astype(F32) * FACTOR_DOWN
    factor = jnp.concatenate([factor, jnp.zeros_like(factor)], axis=0)
    factor = lax.dot(pick_factor, factor, precision=lax.Precision.HIGHEST, preferred_element_type=F32)

    for c in range(forward.shape[0]):
        w = [message[pl.ds(2 * c + t, count, stride=per), :] for t in range(2)]
        byte = [lambda w: w & 255, lambda w: lax.shift_right_logical(w, 8) & 255, lambda w: lax.shift_right_logical(w, 16) & 255]
        parts = [[(f(v) - 128) for v in w] for f in byte] + [[lax.shift_right_arithmetic(v, 24) for v in w]]
        parts = [[v.astype(F32).astype(jnp.bfloat16) for v in p] for p in parts]
        low = jnp.concatenate(parts[0] + parts[1], axis=1)
        high = jnp.concatenate(parts[2] + parts[3], axis=1)
        table = jnp.concatenate([low, high], axis=0)
        picked = lax.dot(pick, table, preferred_element_type=F32)
        forward[c] = picked * factor[:, c : c + 1]
    for n in (0, 2, 3, 4):
        copies[n].wait()
    last = cells_x - 1
    below, above = below_above(far, near)
    prior_y, next_y = prior_next(first, second)
    for x in range(cells_x):
        e = strain_plane(
            v[0, x], v[0, x - 1] if x > 0 else below(0), next_y[0, x : x + 1],
            v[1, x], v[1, x + 1] if x < last else above(0), prior_y[0, x : x + 1],
            v[2, x], v[2, x + 1] if x < last else above(1), next_y[1, x : x + 1],
        )
        new = stress_plane([stress[k, x] for k in range(6)], e, lam[x], mu[x])
        for k in range(6):
            strain2[k, x] = e[k]
            stress[k, x] = new[k]
    results = load(((stress, out.at[pl.ds(3, 6)]),), sems)
    copies[5].wait()
    for step, strain in enumerate((strain1, strain2)):
        f = [forward[6 * step + n] for n in range(6)]
        e = [strain[n].reshape(rows, cells_z) for n in range(6)]
        add_lambda = (e[0] + e[1] + e[2]) * (f[0] + f[1] + f[2])
        add_mu = 2.0 * (e[0] * f[0] + e[1] * f[1] + e[2] * f[2])
        grad_lambda = add_lambda if step == 0 else grad_lambda + add_lambda
        grad_mu = add_mu if step == 0 else grad_mu + add_mu
        grad_mu = grad_mu + e[3] * f[3] + e[4] * f[4] + e[5] * f[5]
    grads[0] = grad_lambda.reshape(cells_x, cells_y, cells_z)
    grads[1] = grad_mu.reshape(cells_x, cells_y, cells_z)
    results += load(((grads, out_grads),), sems.at[pl.ds(1, 1)])
    for copy in results:
        copy.wait()


def on_device(adjoint, buoyancy, lame_lambda, shear_mu, packed, scales, perm):
    cells_x, cells_y, cells_z = buoyancy.shape
    owners, comp, width = packed.shape[1], packed.shape[3], packed.shape[4]
    per = comp * width // 128

    def shape(*dims, dtype=F32):
        return jax.ShapeDtypeStruct(dims, dtype)

    def in_hbm(*values):
        return [pltpu.with_memory_space_constraint(value, pltpu.HBM) for value in values]

    def call(kernel, mebibytes, outs, args, in_specs=None, scratch=(), out_specs=None, aliases={}):
        return pl.pallas_call(
            kernel,
            out_shape=outs,
            in_specs=in_specs or [VMEM] * len(args),
            out_specs=out_specs or (VMEM,) * len(outs),
            scratch_shapes=scratch,
            compiler_params=pltpu.CompilerParams(vmem_limit_bytes=mebibytes << 20),
            input_output_aliases=aliases,
        )(*args)

    count_x = lax.axis_size("gx")
    count_y = lax.axis_size("gy")
    off_chip = [(x, x + 1 if x % 2 else x - 1) for x in range(1, count_x - 1)]
    on_chip = [(x, x ^ 1) for x in range(count_x)]
    pairs = [[(y, y + 1) for y in range(start, count_y - 1, 2)] for start in (0, 1)]
    pairs = [[*there, *((b, a) for a, b in there)] for there in pairs]

    def swap(far, near, first, second):
        far = lax.ppermute(far, "gx", off_chip)
        near = lax.ppermute(near, "gx", on_chip)
        first = lax.ppermute(first, "gy", pairs[0])
        second = lax.ppermute(second, "gy", pairs[1])
        return far, near, first, second

    def planes(*count):
        return shape(*count, cells_y, cells_z)

    def lines(count):
        return shape(count, cells_x, cells_z)

    sent = call(
        prepare, 8, (planes(2), planes(2), lines(len(DOWN_ROWS)), lines(len(DOWN_ROWS))),
        in_hbm(adjoint, buoyancy, lame_lambda, shear_mu), [ANY] * 4,
        [
            pltpu.VMEM((len(UP_ROWS) + len(DOWN_ROWS), cells_x, 8, cells_z), F32),
            pltpu.SemaphoreType.DMA((6,)),
            pltpu.SemaphoreType.DMA((len(UP_ROWS) + len(DOWN_ROWS),)),
        ],
    )
    s_ghosts = swap(*sent)

    by_comp = jnp.transpose(scales.reshape(owners, comp)).reshape(comp, 1, owners)
    size = (owners * (per + 1), 128)
    (message,) = call(
        merge, 8, (pltpu.HBM(size, jnp.int32),), (*in_hbm(packed.reshape(owners * per, 128)), by_comp), [ANY, VMEM],
        [
            pltpu.VMEM((owners * per, 128), jnp.int32), pltpu.VMEM(size, jnp.int32),
            pltpu.SemaphoreType.DMA((4,)), pltpu.SemaphoreType.DMA((4,)),
        ],
        (ANY,),
    )
    message = lax.all_to_all(message.reshape(owners, per + 1, 1, 128), "gx", split_axis=0, concat_axis=0, tiled=True)
    message = message.reshape(owners * (per + 1), 128)

    faces = shape(5 * cells_y + 8, cells_z)
    strain = (6, cells_x, cells_y, cells_z)
    speeds = (3, cells_x, cells_y, cells_z)

    def rooms(*sizes):
        return [pltpu.VMEM(size, F32) for size in sizes]

    def semaphores(*counts):
        return [pltpu.SemaphoreType.DMA((count,)) for count in counts]

    whole = adjoint.shape
    plane = buoyancy.shape[1:]
    pair = (2, *plane)
    ghost_rows = (len(DOWN_ROWS), cells_x, cells_z)
    sent = call(
        first_velocity, 12, (faces, faces, lines(3), lines(3)), (adjoint, buoyancy, *in_hbm(lame_lambda, shear_mu), *s_ghosts),
        [VMEM] * 2 + [ANY] * 2 + [VMEM] * 4, rooms(speeds, (3, *plane)) + semaphores(3),
    )
    v_ghosts = swap(*sent)

    kept = in_hbm(adjoint, buoyancy, lame_lambda, shear_mu, *s_ghosts)
    small = (buoyancy.shape, buoyancy.shape, pair, pair, ghost_rows, ghost_rows)
    sent = call(
        edges, 16, (planes(2), planes(2), lines(2), lines(2)), (*kept, *v_ghosts),
        [ANY] * 8 + [VMEM] * 4, rooms(whole, buoyancy.shape, *small, speeds, strain) + semaphores(8),
    )
    w_ghosts = swap(*sent)
    fields, strain1 = call(
        inner, 24, (pltpu.HBM(whole, F32), pltpu.HBM(strain, F32)), (*kept, *v_ghosts), [ANY] * 8 + [VMEM] * 4,
        rooms(whole, buoyancy.shape, *small, speeds, strain, strain) + semaphores(8, 3), (ANY, ANY),
    )
    grads = (2, *buoyancy.shape)
    adjoint_out, grads = call(
        finish, 24, (pltpu.HBM(whole, F32), pltpu.HBM(grads, F32)),
        (*in_hbm(fields, lame_lambda, shear_mu, strain1, perm), *w_ghosts, message), [ANY] * 5 + [VMEM] * 5,
        rooms(speeds, strain, buoyancy.shape, buoyancy.shape, strain) + [pltpu.VMEM(perm.shape, jnp.int32)]
        + rooms(strain, (comp, cells_x * cells_y, cells_z), grads) + semaphores(6, 2),
        (ANY, ANY), {0: 0},
    )
    return adjoint_out, grads


def solution(mesh):
    return jax.shard_map(
        on_device,
        mesh=mesh,
        in_specs=(
            P(None, "gx", "gy", None),
            P("gx", "gy", None),
            P("gx", "gy", None),
            P("gx", "gy", None),
            P("gx", None, "gy", None, None),
            P("gx", None, "gy", None),
            P("gx", None),
        ),
        out_specs=(P(None, "gx", "gy", None), P(None, "gx", "gy", None)),
        check_vma=False,
    )
```

```python
import jax
import jax.numpy as jnp
from jax import lax
from jax.experimental import pallas as pl
from jax.experimental.pallas import tpu as pltpu
from jax.sharding import PartitionSpec as P


courant = 0.15
FACTOR_UP = 2.0**35
FACTOR_DOWN = 2.0**-35
F32 = jnp.float32
ANY = pl.BlockSpec(memory_space=pl.ANY)
VMEM = pl.BlockSpec(memory_space=pltpu.VMEM)


def below_y(field, row):
    y = lax.broadcasted_iota(jnp.int32, field.shape, 0)
    return jnp.where(y == 0, row, pltpu.roll(field, 1, 0))


def above_y(field, row):
    count = field.shape[0]
    y = lax.broadcasted_iota(jnp.int32, field.shape, 0)
    return jnp.where(y == count - 1, row, pltpu.roll(field, count - 1, 0))


def below_z(field):
    z = lax.broadcasted_iota(jnp.int32, field.shape, 1)
    return jnp.where(z == 0, 0.0, pltpu.roll(field, 1, 1))


def above_z(field):
    count = field.shape[1]
    z = lax.broadcasted_iota(jnp.int32, field.shape, 1)
    return jnp.where(z == count - 1, 0.0, pltpu.roll(field, count - 1, 1))


def velocity_plane(vel, scaled, sxx, sxx_next, syy, syy_row, szz, sxy, sxy_prior, sxy_row, sxz, sxz_prior, syz, syz_row):
    vx, vy, vz = vel
    vx = vx - scaled * (sxx_next - sxx + (sxy - below_y(sxy, sxy_row)) + (sxz - below_z(sxz)))
    vy = vy - scaled * (sxy - sxy_prior + (above_y(syy, syy_row) - syy) + (syz - below_z(syz)))
    vz = vz - scaled * (sxz - sxz_prior + (syz - below_y(syz, syz_row)) + (above_z(szz) - szz))
    return vx, vy, vz


def strain_plane(vx, vx_prior, vx_row, vy, vy_next, vy_row, vz, vz_next, vz_row):
    exx = vx - vx_prior
    eyy = vy - below_y(vy, vy_row)
    ezz = vz - below_z(vz)
    exy = (above_y(vx, vx_row) - vx) + (vy_next - vy)
    exz = (above_z(vx) - vx) + (vz_next - vz)
    eyz = (above_z(vy) - vy) + (above_y(vz, vz_row) - vz)
    return exx, eyy, ezz, exy, exz, eyz


def stress_plane(stress, strain, lam, mu):
    trace = strain[0] + strain[1] + strain[2]
    direct = [stress[k] - courant * (lam * trace + 2.0 * mu * strain[k]) for k in range(3)]
    shear = [stress[k] - courant * mu * strain[k] for k in range(3, 6)]
    return direct + shear


UP_ROWS = tuple((n, 1) for n in (0, 1, 2, 3, 4, 5, 6, 7, 8, 9, 11)) + ((6, 2), (8, 2))
DOWN_ROWS = tuple((n, 1) for n in range(12)) + ((4, 2),)
PLANES = 7


def on_lower_core():
    return lax.axis_index("gx") % 2 == 0


def below_above(far, near):
    lower = on_lower_core()
    return lambda k: jnp.where(lower, far[k], near[k]), lambda k: jnp.where(lower, near[k], far[k])


def far_near(up, down):
    lower = on_lower_core()
    return jnp.where(lower, down, up), jnp.where(lower, up, down)


def on_even_row():
    return lax.axis_index("gy") % 2 == 0


def prior_next(first, second):
    even = on_even_row()
    return jnp.where(even, second[...], first[...]), jnp.where(even, first[...], second[...])


def first_second(to_next, to_prior):
    even = on_even_row()
    return jnp.where(even, to_next, to_prior), jnp.where(even, to_prior, to_next)


def prepare(adj, buoy, lam, mu, first, second, rows, sems):
    cells_y = adj.shape[2]
    extra = (buoy, lam, mu)
    plans = []
    for side, start in enumerate((cells_y - 8, 0)):
        plans.append((adj.at[:, :, pl.ds(start, 8)], rows.at[side, pl.ds(0, 9)]))
        plans += [(extra[n].at[:, pl.ds(start, 8)], rows.at[side, 9 + n]) for n in range(3)]
    for copy in load(plans, sems):
        copy.wait()
    for k, ((up, up_depth), (down, down_depth)) in enumerate(zip(UP_ROWS, DOWN_ROWS)):
        first[k], second[k] = first_second(rows[0, up, :, 8 - up_depth, :], rows[1, down, :, down_depth - 1, :])


def merge(packed, scales, message, words, build, word_sems, sems):
    comp, _, count = scales.shape
    per = packed.shape[0] // count
    size = 16
    starts = range(0, count, size)
    loads = []
    for n, start in enumerate(starts):
        part = pl.ds(start * per, size * per)
        loads.append(pltpu.make_async_copy(packed.at[part], words.at[part], word_sems.at[n]))
        loads[-1].start()
    factor = jnp.pad(scales[:, 0, :], ((0, 128 - comp), (0, 128 - count)))
    factor = (jnp.transpose(factor)[:count] * FACTOR_UP).astype(jnp.int32)
    build[pl.ds(per, count, stride=per + 1), :] = factor
    copies = []
    for n, start in enumerate(starts):
        loads[n].wait()
        for r in range(per):
            build[pl.ds(start * (per + 1) + r, size, stride=per + 1), :] = words[pl.ds(start * per + r, size, stride=per), :]
        part = pl.ds(start * (per + 1), size * (per + 1))
        copies.append(pltpu.make_async_copy(build.at[part], message.at[part], sems.at[n]))
        copies[-1].start()
    for copy in copies:
        copy.wait()


def load(plans, sems):
    copies = [pltpu.make_async_copy(source, target, sems.at[n]) for n, (source, target) in enumerate(plans)]
    for copy in copies:
        copy.start()
    return copies


def step_one(adj, buoy, x, sxx_next, sxy_prior, sxz_prior, prior_y, next_y):
    row = slice(x, x + 1)
    return velocity_plane(
        (adj[0, x], adj[1, x], adj[2, x]), courant * buoy[x], adj[3, x], sxx_next, adj[4, x], next_y[4, 1][row], adj[5, x],
        adj[6, x], sxy_prior, prior_y[6, 1][row], adj[7, x], sxz_prior, adj[8, x], prior_y[8, 1][row],
    )


def named_rows(first, second):
    prior_y, next_y = prior_next(first, second)
    return {name: prior_y[k] for k, name in enumerate(UP_ROWS)}, {name: next_y[k] for k, name in enumerate(DOWN_ROWS)}


def places(cells_y):
    return [pl.ds(k * cells_y, cells_y) for k in range(PLANES)], [pl.ds(PLANES * cells_y + k, 1) for k in range(6)]


def reach(adj, buoy, lam, mu, first, second, far, near, planes, sems):
    cells_x, cells_y = adj.shape[1:3]
    last = cells_x - 1
    loads = load(((mu.at[last], planes.at[0]), (lam.at[0], planes.at[1]), (mu.at[0], planes.at[2])), sems)
    prior_y, next_y = named_rows(first, second)
    blank = jnp.zeros_like(adj[0, 0])
    up = [*step_one(adj, buoy, last, blank, adj[6, last - 1], adj[7, last - 1], prior_y, next_y), buoy[last], adj[6, last], adj[7, last]]
    down = [*step_one(adj, buoy, 0, adj[3, 1], blank, blank, prior_y, next_y), buoy[0], adj[3, 0]]
    own = {n: next_y[n, 1][last:] for n in range(10)}
    scaled_up = courant * own[9]
    sides = (own[6] - adj[6, last][cells_y - 1 :, :]) + (own[7] - below_z(own[7]))
    up_rows = [own[0] - scaled_up * (sides - own[3]), scaled_up]
    up_rows += [rows[n, 1][last:] for rows in (prior_y, next_y) for n in (6, 7)]
    own = {n: prior_y[n, 1][0:1] for n in range(10)}
    scaled_down = courant * own[9]
    sides = (adj[4, 0][0:1, :] - own[4]) + (own[8] - below_z(own[8]))
    down_rows = [own[1] - scaled_down * (own[6] + sides), scaled_down, own[3], next_y[3, 1][0:1]]
    down_rows += [jnp.zeros_like(scaled_down)] * 2
    whole, lines = places(cells_y)
    for copy in loads:
        copy.wait()
    up.append(planes[0])
    down += [planes[1], planes[2]]
    for place, a, b in zip(whole + lines, up + up_rows, down + down_rows):
        far[place, :], near[place, :] = far_near(a, b)


def half(adj, buoy, lam, mu, far, near, first, second, v, stress, strain, between):
    cells_x, cells_y = adj.shape[1:3]
    last = cells_x - 1
    from_below, from_above = below_above(far, near)
    prior_y, next_y = named_rows(first, second)
    whole, lines = places(cells_y)
    vx_m, vy_m, vz_m, buoy_m, sxy_m, sxz_m, mu_m = (from_below(place) for place in whole)
    vx_n, vy_n, vz_n, buoy_n, sxx_n, lam_n, mu_n = (from_above(place) for place in whole)
    vx_m = vx_m - courant * buoy_m * adj[3, 0]
    vy_n = vy_n + courant * buoy_n * adj[6, last]
    vz_n = vz_n + courant * buoy_n * adj[7, last]
    for x in range(cells_x):
        new = step_one(
            adj, buoy, x, adj[3, x + 1] if x < last else sxx_n, adj[6, x - 1] if x > 0 else sxy_m, adj[7, x - 1] if x > 0 else sxz_m,
            prior_y, next_y,
        )
        for k in range(3):
            v[k, x] = new[k]
    vx_corner = from_below(lines[0]) - from_below(lines[1]) * next_y[3, 1][0:1]
    vy_corner = from_above(lines[0]) + from_above(lines[1]) * prior_y[6, 1][last:]
    ghosts = []
    for side, here in enumerate((prior_y, next_y)):
        scaled = courant * here[9, 1]
        sxx, syy, szz, sxy, sxz, syz = (here[n, 1] for n in range(3, 9))
        sxx_after = jnp.concatenate([sxx[1:], from_above(lines[2 + side])], axis=0)
        sxy_before = jnp.concatenate([from_below(lines[2 + 2 * side]), sxy[:last]], axis=0)
        sxz_before = jnp.concatenate([from_below(lines[3 + 2 * side]), sxz[:last]], axis=0)
        if side == 0:
            sxy_under, syz_under, syy_over = here[6, 2], here[8, 2], adj[4, :, 0, :]
        else:
            sxy_under, syz_under, syy_over = adj[6, :, cells_y - 1, :], adj[8, :, cells_y - 1, :], here[4, 2]
        ghosts.append([
            here[0, 1] - scaled * (sxx_after - sxx + (sxy - sxy_under) + (sxz - below_z(sxz))),
            here[1, 1] - scaled * (sxy - sxy_before + (syy_over - syy) + (syz - below_z(syz))),
            here[2, 1] - scaled * (sxz - sxz_before + (syz - syz_under) + (above_z(szz) - szz)),
        ])
    v_prior_y, v_next_y = ghosts
    exx = vx_n - v[0, last]
    trace = exx + (vy_n - below_y(vy_n, vy_corner)) + (vz_n - below_z(vz_n))
    sxx_next = sxx_n - courant * (lam_n * trace + 2.0 * mu_n * exx)
    exy = (above_y(vx_m, vx_corner) - vx_m) + (v[1, 0] - vy_m)
    exz = (above_z(vx_m) - vx_m) + (v[2, 0] - vz_m)
    sxy_prior = sxy_m - courant * mu_m * exy
    sxz_prior = sxz_m - courant * mu_m * exz
    over = v_next_y[0]
    exx = over - jnp.concatenate([vx_corner, over[:last]], axis=0)
    eyy = v_next_y[1] - v[1, :, cells_y - 1, :]
    trace = exx + eyy + (v_next_y[2] - below_z(v_next_y[2]))
    syy_rows = next_y[4, 1] - courant * (next_y[10, 1] * trace + 2.0 * next_y[11, 1] * eyy)
    under = v_prior_y[1]
    exy = (v[0, :, 0, :] - v_prior_y[0]) + (jnp.concatenate([under[1:], vy_corner], axis=0) - under)
    eyz = (above_z(under) - under) + (v[2, :, 0, :] - v_prior_y[2])
    sxy_rows = prior_y[6, 1] - courant * prior_y[11, 1] * exy
    syz_rows = prior_y[8, 1] - courant * prior_y[11, 1] * eyz
    for x in range(cells_x):
        e = strain_plane(
            v[0, x], v[0, x - 1] if x > 0 else vx_m, v_next_y[0][x : x + 1],
            v[1, x], v[1, x + 1] if x < last else vy_n, v_prior_y[1][x : x + 1],
            v[2, x], v[2, x + 1] if x < last else vz_n, v_next_y[2][x : x + 1],
        )
        s = stress_plane([adj[3 + k, x] for k in range(6)], e, lam[x], mu[x])
        for k in range(6):
            stress[k, x] = s[k]
            if strain is not None:
                strain[k, x] = e[k]
    between()
    for x in range(cells_x):
        new = velocity_plane(
            (v[0, x], v[1, x], v[2, x]), courant * buoy[x],
            stress[0, x], stress[0, x + 1] if x < last else sxx_next, stress[1, x], syy_rows[x : x + 1], stress[2, x],
            stress[3, x], stress[3, x - 1] if x > 0 else sxy_prior, sxy_rows[x : x + 1],
            stress[4, x], stress[4, x - 1] if x > 0 else sxz_prior, stress[5, x], syz_rows[x : x + 1],
        )
        for k in range(3):
            v[k, x] = new[k]


def edges(
    adj_in, buoy_in, lam_in, mu_in, far_in, near_in, first_in, second_in, far, near, first, second,
    adj, buoy, lam, mu, far_here, near_here, first_here, second_here, v, stress, sems,
):
    given = (adj_in, buoy_in, lam_in, mu_in, far_in, near_in, first_in, second_in)
    here = (adj, buoy, lam, mu, far_here, near_here, first_here, second_here)
    for copy in load(zip(given, here), sems):
        copy.wait()
    half(*here, v, stress, None, lambda: None)
    _, cells_x, cells_y, _ = v.shape
    over, under = v[1, :, cells_y - 1, :], v[0, :, 0, :]
    first[0], second[0] = first_second(over, under)
    under = v[2, :, 0, :]
    first[1], second[1] = first_second(jnp.zeros_like(under), under)
    far[0], near[0] = far_near(v[0, cells_x - 1], v[1, 0])
    far[1], near[1] = far_near(jnp.zeros_like(v[2, 0]), v[2, 0])


def inner(
    adj_in, buoy_in, lam_in, mu_in, far_in, near_in, first_in, second_in, fields, strain_out,
    adj, buoy, lam, mu, far, near, first, second, v, stress, strain, load_sems, sems,
):
    given = (adj_in, buoy_in, lam_in, mu_in, far_in, near_in, first_in, second_in)
    here = (adj, buoy, lam, mu, far, near, first, second)
    for copy in load(zip(given, here), load_sems):
        copy.wait()
    copies = [
        pltpu.make_async_copy(strain, strain_out, sems.at[0]),
        pltpu.make_async_copy(stress, fields.at[pl.ds(3, 6)], sems.at[1]),
        pltpu.make_async_copy(v, fields.at[pl.ds(0, 3)], sems.at[2]),
    ]
    half(*here, v, stress, strain, lambda: [copy.start() for copy in copies[:2]])
    copies[2].start()
    for copy in copies:
        copy.wait()


def finish(
    fields, lam_in, mu_in, strain_in, perm_in, far, near, first, second, message, out, out_grads,
    v, stress, lam, mu, strain1, perm, strain2, forward, grads, load_sems, sems,
):
    cells_x, cells_y, cells_z = strain1.shape[1:]
    plans = (
        (fields.at[pl.ds(0, 3)], v), (perm_in, perm), (fields.at[pl.ds(3, 6)], stress), (lam_in, lam), (mu_in, mu), (strain_in, strain1),
    )
    copies = load(plans, load_sems)
    count = perm.shape[1]
    per = message.shape[0] // count
    rows = cells_x * cells_y
    copies[1].wait()
    both = jnp.concatenate([perm[...], perm[...]], axis=1)
    r = lax.broadcasted_iota(jnp.int32, (rows, 2 * count), 0)
    k = lax.broadcasted_iota(jnp.int32, (rows, 2 * count), 1)
    mine = both == lax.shift_right_logical(r, 1)
    half = (k >= count) == ((r & 1) == 1)
    pick = jnp.where(mine & half, 1.0, 0.0).astype(jnp.bfloat16)
    pick_factor = jnp.where(mine & (k < count), 1.0, 0.0)
    factor = message[pl.ds(per - 1, count, stride=per), :].astype(F32) * FACTOR_DOWN
    factor = jnp.concatenate([factor, jnp.zeros_like(factor)], axis=0)
    factor = lax.dot(pick_factor, factor, precision=lax.Precision.HIGHEST, preferred_element_type=F32)

    for c in range(forward.shape[0]):
        w = [message[pl.ds(2 * c + t, count, stride=per), :] for t in range(2)]
        byte = [lambda w: w & 255, lambda w: lax.shift_right_logical(w, 8) & 255, lambda w: lax.shift_right_logical(w, 16) & 255]
        parts = [[(f(v) - 128) for v in w] for f in byte] + [[lax.shift_right_arithmetic(v, 24) for v in w]]
        parts = [[v.astype(F32).astype(jnp.bfloat16) for v in p] for p in parts]
        low = jnp.concatenate(parts[0] + parts[1], axis=1)
        high = jnp.concatenate(parts[2] + parts[3], axis=1)
        table = jnp.concatenate([low, high], axis=0)
        picked = lax.dot(pick, table, preferred_element_type=F32)
        forward[c] = picked * factor[:, c : c + 1]
    for n in (0, 2, 3, 4):
        copies[n].wait()
    last = cells_x - 1
    below, above = below_above(far, near)
    prior_y, next_y = prior_next(first, second)
    for x in range(cells_x):
        e = strain_plane(
            v[0, x], v[0, x - 1] if x > 0 else below(0), next_y[0, x : x + 1],
            v[1, x], v[1, x + 1] if x < last else above(0), prior_y[0, x : x + 1],
            v[2, x], v[2, x + 1] if x < last else above(1), next_y[1, x : x + 1],
        )
        new = stress_plane([stress[k, x] for k in range(6)], e, lam[x], mu[x])
        for k in range(6):
            strain2[k, x] = e[k]
            stress[k, x] = new[k]
    results = load(((stress, out.at[pl.ds(3, 6)]),), sems)
    copies[5].wait()
    for step, strain in enumerate((strain1, strain2)):
        f = [forward[6 * step + n] for n in range(6)]
        e = [strain[n].reshape(rows, cells_z) for n in range(6)]
        add_lambda = (e[0] + e[1] + e[2]) * (f[0] + f[1] + f[2])
        add_mu = 2.0 * (e[0] * f[0] + e[1] * f[1] + e[2] * f[2])
        grad_lambda = add_lambda if step == 0 else grad_lambda + add_lambda
        grad_mu = add_mu if step == 0 else grad_mu + add_mu
        grad_mu = grad_mu + e[3] * f[3] + e[4] * f[4] + e[5] * f[5]
    grads[0] = grad_lambda.reshape(cells_x, cells_y, cells_z)
    grads[1] = grad_mu.reshape(cells_x, cells_y, cells_z)
    results += load(((grads, out_grads),), sems.at[pl.ds(1, 1)])
    for copy in results:
        copy.wait()


def on_device(adjoint, buoyancy, lame_lambda, shear_mu, packed, scales, perm):
    cells_x, cells_y, cells_z = buoyancy.shape
    owners, comp, width = packed.shape[1], packed.shape[3], packed.shape[4]
    per = comp * width // 128

    def shape(*dims, dtype=F32):
        return jax.ShapeDtypeStruct(dims, dtype)

    def in_hbm(*values):
        return [pltpu.with_memory_space_constraint(value, pltpu.HBM) for value in values]

    def call(kernel, mebibytes, outs, args, in_specs=None, scratch=(), out_specs=None, aliases={}):
        return pl.pallas_call(
            kernel,
            out_shape=outs,
            in_specs=in_specs or [VMEM] * len(args),
            out_specs=out_specs or (VMEM,) * len(outs),
            scratch_shapes=scratch,
            compiler_params=pltpu.CompilerParams(vmem_limit_bytes=mebibytes << 20),
            input_output_aliases=aliases,
        )(*args)

    count_x = lax.axis_size("gx")
    count_y = lax.axis_size("gy")
    off_chip = [(x, x + 1 if x % 2 else x - 1) for x in range(1, count_x - 1)]
    on_chip = [(x, x ^ 1) for x in range(count_x)]
    pairs = [[(y, y + 1) for y in range(start, count_y - 1, 2)] for start in (0, 1)]
    pairs = [[*there, *((b, a) for a, b in there)] for there in pairs]

    def planes(*count):
        return shape(*count, cells_y, cells_z)

    def lines(count):
        return shape(count, cells_x, cells_z)

    def rooms(*sizes):
        return [pltpu.VMEM(size, F32) for size in sizes]

    def semaphores(*counts):
        return [pltpu.SemaphoreType.DMA((count,)) for count in counts]

    raw = in_hbm(adjoint, buoyancy, lame_lambda, shear_mu)
    first, second = call(
        prepare, 8, (lines(len(UP_ROWS)), lines(len(UP_ROWS))), raw, [ANY] * 4, rooms((2, 12, cells_x, 8, cells_z)) + semaphores(8)
    )
    first = lax.ppermute(first, "gy", pairs[0])
    second = lax.ppermute(second, "gy", pairs[1])

    by_comp = jnp.transpose(scales.reshape(owners, comp)).reshape(comp, 1, owners)
    size = (owners * (per + 1), 128)
    (message,) = call(
        merge, 8, (pltpu.HBM(size, jnp.int32),), (*in_hbm(packed.reshape(owners * per, 128)), by_comp), [ANY, VMEM],
        [
            pltpu.VMEM((owners * per, 128), jnp.int32), pltpu.VMEM(size, jnp.int32),
            pltpu.SemaphoreType.DMA((4,)), pltpu.SemaphoreType.DMA((4,)),
        ],
        (ANY,),
    )
    message = lax.all_to_all(message.reshape(owners, per + 1, 1, 128), "gx", split_axis=0, concat_axis=0, tiled=True)
    message = message.reshape(owners * (per + 1), 128)

    whole = adjoint.shape
    strain = (6, *buoyancy.shape)
    speeds = (3, *buoyancy.shape)
    message_rows = (PLANES * cells_y + 8, cells_z)
    faces = shape(*message_rows)
    far, near = call(
        reach, 12, (faces, faces), (adjoint, buoyancy, *raw[2:], first, second), [VMEM] * 2 + [ANY] * 2 + [VMEM] * 2,
        rooms((3, cells_y, cells_z)) + semaphores(3),
    )
    far = lax.ppermute(far, "gx", off_chip)
    near = lax.ppermute(near, "gx", on_chip)

    given = (*raw, *in_hbm(far, near, first, second))
    line_rows = (len(UP_ROWS), cells_x, cells_z)
    here = (whole, *[buoyancy.shape] * 3, message_rows, message_rows, line_rows, line_rows)
    far, near, first, second = call(
        edges, 16, (planes(2), planes(2), lines(2), lines(2)), given, [ANY] * 8, rooms(*here, speeds, strain) + semaphores(8)
    )
    w_ghosts = (
        lax.ppermute(far, "gx", off_chip), lax.ppermute(near, "gx", on_chip),
        lax.ppermute(first, "gy", pairs[0]), lax.ppermute(second, "gy", pairs[1]),
    )
    fields, strain1 = call(
        inner, 24, (pltpu.HBM(whole, F32), pltpu.HBM(strain, F32)), given, [ANY] * 8,
        rooms(*here, speeds, strain, strain) + semaphores(8, 3), (ANY, ANY),
    )
    grads = (2, *buoyancy.shape)
    adjoint_out, grads = call(
        finish, 24, (pltpu.HBM(whole, F32), pltpu.HBM(grads, F32)),
        (*in_hbm(fields, lame_lambda, shear_mu, strain1, perm), *w_ghosts, message), [ANY] * 5 + [VMEM] * 5,
        rooms(speeds, strain, buoyancy.shape, buoyancy.shape, strain) + [pltpu.VMEM(perm.shape, jnp.int32)]
        + rooms(strain, (comp, cells_x * cells_y, cells_z), grads) + semaphores(6, 2),
        (ANY, ANY), {0: 0},
    )
    return adjoint_out, grads


def solution(mesh):
    return jax.shard_map(
        on_device,
        mesh=mesh,
        in_specs=(
            P(None, "gx", "gy", None),
            P("gx", "gy", None),
            P("gx", "gy", None),
            P("gx", "gy", None),
            P("gx", None, "gy", None, None),
            P("gx", None, "gy", None),
            P("gx", None),
        ),
        out_specs=(P(None, "gx", "gy", None), P(None, "gx", "gy", None)),
        check_vma=False,
    )
```

```python
import jax
import jax.numpy as jnp
from jax import lax
from jax.experimental import pallas as pl
from jax.experimental.pallas import tpu as pltpu
from jax.sharding import PartitionSpec as P


courant = 0.15
FACTOR_UP = 2.0**35
FACTOR_DOWN = 2.0**-35
F32 = jnp.float32
ANY = pl.BlockSpec(memory_space=pl.ANY)
VMEM = pl.BlockSpec(memory_space=pltpu.VMEM)


def below_y(field, row):
    y = lax.broadcasted_iota(jnp.int32, field.shape, 0)
    return jnp.where(y == 0, row, pltpu.roll(field, 1, 0))


def above_y(field, row):
    count = field.shape[0]
    y = lax.broadcasted_iota(jnp.int32, field.shape, 0)
    return jnp.where(y == count - 1, row, pltpu.roll(field, count - 1, 0))


def below_z(field):
    z = lax.broadcasted_iota(jnp.int32, field.shape, 1)
    return jnp.where(z == 0, 0.0, pltpu.roll(field, 1, 1))


def above_z(field):
    count = field.shape[1]
    z = lax.broadcasted_iota(jnp.int32, field.shape, 1)
    return jnp.where(z == count - 1, 0.0, pltpu.roll(field, count - 1, 1))


def velocity_plane(vel, scaled, sxx, sxx_next, syy, syy_row, szz, sxy, sxy_prior, sxy_row, sxz, sxz_prior, syz, syz_row):
    vx, vy, vz = vel
    vx = vx - scaled * (sxx_next - sxx + (sxy - below_y(sxy, sxy_row)) + (sxz - below_z(sxz)))
    vy = vy - scaled * (sxy - sxy_prior + (above_y(syy, syy_row) - syy) + (syz - below_z(syz)))
    vz = vz - scaled * (sxz - sxz_prior + (syz - below_y(syz, syz_row)) + (above_z(szz) - szz))
    return vx, vy, vz


def strain_plane(vx, vx_prior, vx_row, vy, vy_next, vy_row, vz, vz_next, vz_row):
    exx = vx - vx_prior
    eyy = vy - below_y(vy, vy_row)
    ezz = vz - below_z(vz)
    exy = (above_y(vx, vx_row) - vx) + (vy_next - vy)
    exz = (above_z(vx) - vx) + (vz_next - vz)
    eyz = (above_z(vy) - vy) + (above_y(vz, vz_row) - vz)
    return exx, eyy, ezz, exy, exz, eyz


def stress_plane(stress, strain, lam, mu):
    trace = strain[0] + strain[1] + strain[2]
    direct = [stress[k] - courant * (lam * trace + 2.0 * mu * strain[k]) for k in range(3)]
    shear = [stress[k] - courant * mu * strain[k] for k in range(3, 6)]
    return direct + shear


UP_ROWS = tuple((n, 1) for n in (0, 1, 2, 3, 4, 5, 6, 7, 8, 9, 11)) + ((6, 2), (8, 2))
DOWN_ROWS = tuple((n, 1) for n in range(12)) + ((4, 2),)
PLANES = 7


def on_lower_core():
    return lax.axis_index("gx") % 2 == 0


def below_above(far, near):
    lower = on_lower_core()
    return lambda k: jnp.where(lower, far[k], near[k]), lambda k: jnp.where(lower, near[k], far[k])


def far_near(up, down):
    lower = on_lower_core()
    return jnp.where(lower, down, up), jnp.where(lower, up, down)


def on_even_row():
    return lax.axis_index("gy") % 2 == 0


def prior_next(first, second):
    even = on_even_row()
    return jnp.where(even, second[...], first[...]), jnp.where(even, first[...], second[...])


def first_second(to_next, to_prior):
    even = on_even_row()
    return jnp.where(even, to_next, to_prior), jnp.where(even, to_prior, to_next)


def prepare(adj, buoy, lam, mu, first, second, rows, sems):
    cells_y = adj.shape[2]
    extra = (buoy, lam, mu)
    plans = []
    for side, start in enumerate((cells_y - 8, 0)):
        plans.append((adj.at[:, :, pl.ds(start, 8)], rows.at[side, pl.ds(0, 9)]))
        plans += [(extra[n].at[:, pl.ds(start, 8)], rows.at[side, 9 + n]) for n in range(3)]
    for copy in load(plans, sems):
        copy.wait()
    for k, ((up, up_depth), (down, down_depth)) in enumerate(zip(UP_ROWS, DOWN_ROWS)):
        first[k], second[k] = first_second(rows[0, up, :, 8 - up_depth, :], rows[1, down, :, down_depth - 1, :])


def merge(packed, scales, message, words, build, word_sems, sems):
    comp, _, count = scales.shape
    per = packed.shape[0] // count
    size = 16
    starts = range(0, count, size)
    loads = []
    for n, start in enumerate(starts):
        part = pl.ds(start * per, size * per)
        loads.append(pltpu.make_async_copy(packed.at[part], words.at[part], word_sems.at[n]))
        loads[-1].start()
    factor = jnp.pad(scales[:, 0, :], ((0, 128 - comp), (0, 128 - count)))
    factor = (jnp.transpose(factor)[:count] * FACTOR_UP).astype(jnp.int32)
    build[pl.ds(per, count, stride=per + 1), :] = factor
    copies = []
    for n, start in enumerate(starts):
        loads[n].wait()
        for r in range(per):
            build[pl.ds(start * (per + 1) + r, size, stride=per + 1), :] = words[pl.ds(start * per + r, size, stride=per), :]
        part = pl.ds(start * (per + 1), size * (per + 1))
        copies.append(pltpu.make_async_copy(build.at[part], message.at[part], sems.at[n]))
        copies[-1].start()
    for copy in copies:
        copy.wait()


def load(plans, sems):
    copies = [pltpu.make_async_copy(source, target, sems.at[n]) for n, (source, target) in enumerate(plans)]
    for copy in copies:
        copy.start()
    return copies


def step_one(adj, buoy, x, sxx_next, sxy_prior, sxz_prior, prior_y, next_y):
    row = slice(x, x + 1)
    return velocity_plane(
        (adj[0, x], adj[1, x], adj[2, x]), courant * buoy[x], adj[3, x], sxx_next, adj[4, x], next_y[4, 1][row], adj[5, x],
        adj[6, x], sxy_prior, prior_y[6, 1][row], adj[7, x], sxz_prior, adj[8, x], prior_y[8, 1][row],
    )


def named_rows(first, second):
    prior_y, next_y = prior_next(first, second)
    return {name: prior_y[k] for k, name in enumerate(UP_ROWS)}, {name: next_y[k] for k, name in enumerate(DOWN_ROWS)}


def places(cells_y):
    return [pl.ds(k * cells_y, cells_y) for k in range(PLANES)], [pl.ds(PLANES * cells_y + k, 1) for k in range(6)]


def reach(adj, buoy, lam, mu, first, second, far, near, planes, sems):
    cells_x, cells_y = adj.shape[1:3]
    last = cells_x - 1
    loads = load(((mu.at[last], planes.at[0]), (lam.at[0], planes.at[1]), (mu.at[0], planes.at[2])), sems)
    prior_y, next_y = named_rows(first, second)
    blank = jnp.zeros_like(adj[0, 0])
    up = [*step_one(adj, buoy, last, blank, adj[6, last - 1], adj[7, last - 1], prior_y, next_y), buoy[last], adj[6, last], adj[7, last]]
    down = [*step_one(adj, buoy, 0, adj[3, 1], blank, blank, prior_y, next_y), buoy[0], adj[3, 0]]
    own = {n: next_y[n, 1][last:] for n in range(10)}
    scaled_up = courant * own[9]
    sides = (own[6] - adj[6, last][cells_y - 1 :, :]) + (own[7] - below_z(own[7]))
    up_rows = [own[0] - scaled_up * (sides - own[3]), scaled_up]
    up_rows += [rows[n, 1][last:] for rows in (prior_y, next_y) for n in (6, 7)]
    own = {n: prior_y[n, 1][0:1] for n in range(10)}
    scaled_down = courant * own[9]
    sides = (adj[4, 0][0:1, :] - own[4]) + (own[8] - below_z(own[8]))
    down_rows = [own[1] - scaled_down * (own[6] + sides), scaled_down, own[3], next_y[3, 1][0:1]]
    down_rows += [jnp.zeros_like(scaled_down)] * 2
    whole, lines = places(cells_y)
    for copy in loads:
        copy.wait()
    up.append(planes[0])
    down += [planes[1], planes[2]]
    for place, a, b in zip(whole + lines, up + up_rows, down + down_rows):
        far[place, :], near[place, :] = far_near(a, b)


def half(adj, buoy, lam, mu, far, near, first, second, v, stress, strain, between):
    cells_x, cells_y = adj.shape[1:3]
    last = cells_x - 1
    from_below, from_above = below_above(far, near)
    prior_y, next_y = named_rows(first, second)
    whole, lines = places(cells_y)
    vx_m, vy_m, vz_m, buoy_m, sxy_m, sxz_m, mu_m = (from_below(place) for place in whole)
    vx_n, vy_n, vz_n, buoy_n, sxx_n, lam_n, mu_n = (from_above(place) for place in whole)
    vx_m = vx_m - courant * buoy_m * adj[3, 0]
    vy_n = vy_n + courant * buoy_n * adj[6, last]
    vz_n = vz_n + courant * buoy_n * adj[7, last]
    for x in range(cells_x):
        new = step_one(
            adj, buoy, x, adj[3, x + 1] if x < last else sxx_n, adj[6, x - 1] if x > 0 else sxy_m, adj[7, x - 1] if x > 0 else sxz_m,
            prior_y, next_y,
        )
        for k in range(3):
            v[k, x] = new[k]
    vx_corner = from_below(lines[0]) - from_below(lines[1]) * next_y[3, 1][0:1]
    vy_corner = from_above(lines[0]) + from_above(lines[1]) * prior_y[6, 1][last:]
    ghosts = []
    for side, here in enumerate((prior_y, next_y)):
        scaled = courant * here[9, 1]
        sxx, syy, szz, sxy, sxz, syz = (here[n, 1] for n in range(3, 9))
        sxx_after = jnp.concatenate([sxx[1:], from_above(lines[2 + side])], axis=0)
        sxy_before = jnp.concatenate([from_below(lines[2 + 2 * side]), sxy[:last]], axis=0)
        sxz_before = jnp.concatenate([from_below(lines[3 + 2 * side]), sxz[:last]], axis=0)
        if side == 0:
            sxy_under, syz_under, syy_over = here[6, 2], here[8, 2], adj[4, :, 0, :]
        else:
            sxy_under, syz_under, syy_over = adj[6, :, cells_y - 1, :], adj[8, :, cells_y - 1, :], here[4, 2]
        ghosts.append([
            here[0, 1] - scaled * (sxx_after - sxx + (sxy - sxy_under) + (sxz - below_z(sxz))),
            here[1, 1] - scaled * (sxy - sxy_before + (syy_over - syy) + (syz - below_z(syz))),
            here[2, 1] - scaled * (sxz - sxz_before + (syz - syz_under) + (above_z(szz) - szz)),
        ])
    v_prior_y, v_next_y = ghosts
    exx = vx_n - v[0, last]
    trace = exx + (vy_n - below_y(vy_n, vy_corner)) + (vz_n - below_z(vz_n))
    sxx_next = sxx_n - courant * (lam_n * trace + 2.0 * mu_n * exx)
    exy = (above_y(vx_m, vx_corner) - vx_m) + (v[1, 0] - vy_m)
    exz = (above_z(vx_m) - vx_m) + (v[2, 0] - vz_m)
    sxy_prior = sxy_m - courant * mu_m * exy
    sxz_prior = sxz_m - courant * mu_m * exz
    over = v_next_y[0]
    exx = over - jnp.concatenate([vx_corner, over[:last]], axis=0)
    eyy = v_next_y[1] - v[1, :, cells_y - 1, :]
    trace = exx + eyy + (v_next_y[2] - below_z(v_next_y[2]))
    syy_rows = next_y[4, 1] - courant * (next_y[10, 1] * trace + 2.0 * next_y[11, 1] * eyy)
    under = v_prior_y[1]
    exy = (v[0, :, 0, :] - v_prior_y[0]) + (jnp.concatenate([under[1:], vy_corner], axis=0) - under)
    eyz = (above_z(under) - under) + (v[2, :, 0, :] - v_prior_y[2])
    sxy_rows = prior_y[6, 1] - courant * prior_y[11, 1] * exy
    syz_rows = prior_y[8, 1] - courant * prior_y[11, 1] * eyz
    for x in range(cells_x):
        e = strain_plane(
            v[0, x], v[0, x - 1] if x > 0 else vx_m, v_next_y[0][x : x + 1],
            v[1, x], v[1, x + 1] if x < last else vy_n, v_prior_y[1][x : x + 1],
            v[2, x], v[2, x + 1] if x < last else vz_n, v_next_y[2][x : x + 1],
        )
        s = stress_plane([adj[3 + k, x] for k in range(6)], e, lam[x], mu[x])
        for k in range(6):
            stress[k, x] = s[k]
            if strain is not None:
                strain[k, x] = e[k]
    between()
    for x in range(cells_x):
        new = velocity_plane(
            (v[0, x], v[1, x], v[2, x]), courant * buoy[x],
            stress[0, x], stress[0, x + 1] if x < last else sxx_next, stress[1, x], syy_rows[x : x + 1], stress[2, x],
            stress[3, x], stress[3, x - 1] if x > 0 else sxy_prior, sxy_rows[x : x + 1],
            stress[4, x], stress[4, x - 1] if x > 0 else sxz_prior, stress[5, x], syz_rows[x : x + 1],
        )
        for k in range(3):
            v[k, x] = new[k]


def middle(
    adj_in, buoy_in, lam_in, mu_in, far_in, near_in, first_in, second_in, fields, strain_out, far, near, first, second,
    adj, buoy, lam, mu, v, stress, strain, load_sems, sems,
):
    here = (adj, buoy, lam, mu)
    for copy in load(zip((adj_in, buoy_in, lam_in, mu_in), here), load_sems):
        copy.wait()
    copies = [
        pltpu.make_async_copy(strain, strain_out, sems.at[0]),
        pltpu.make_async_copy(stress, fields.at[pl.ds(3, 6)], sems.at[1]),
        pltpu.make_async_copy(v, fields.at[pl.ds(0, 3)], sems.at[2]),
    ]
    half(*here, far_in, near_in, first_in, second_in, v, stress, strain, lambda: [copy.start() for copy in copies[:2]])
    copies[2].start()
    _, cells_x, cells_y, _ = v.shape
    over, under = v[1, :, cells_y - 1, :], v[0, :, 0, :]
    first[0], second[0] = first_second(over, under)
    under = v[2, :, 0, :]
    first[1], second[1] = first_second(jnp.zeros_like(under), under)
    far[0], near[0] = far_near(v[0, cells_x - 1], v[1, 0])
    far[1], near[1] = far_near(jnp.zeros_like(v[2, 0]), v[2, 0])
    for copy in copies:
        copy.wait()


def finish(
    fields, lam_in, mu_in, strain_in, perm_in, far, near, first, second, message, out, out_grads,
    v, stress, lam, mu, strain1, perm, strain2, forward, grads, load_sems, sems,
):
    cells_x, cells_y, cells_z = strain1.shape[1:]
    plans = (
        (fields.at[pl.ds(0, 3)], v), (perm_in, perm), (fields.at[pl.ds(3, 6)], stress), (lam_in, lam), (mu_in, mu), (strain_in, strain1),
    )
    copies = load(plans, load_sems)
    count = perm.shape[1]
    per = message.shape[0] // count
    rows = cells_x * cells_y
    copies[1].wait()
    both = jnp.concatenate([perm[...], perm[...]], axis=1)
    r = lax.broadcasted_iota(jnp.int32, (rows, 2 * count), 0)
    k = lax.broadcasted_iota(jnp.int32, (rows, 2 * count), 1)
    mine = both == lax.shift_right_logical(r, 1)
    half = (k >= count) == ((r & 1) == 1)
    pick = jnp.where(mine & half, 1.0, 0.0).astype(jnp.bfloat16)
    pick_factor = jnp.where(mine & (k < count), 1.0, 0.0)
    factor = message[pl.ds(per - 1, count, stride=per), :].astype(F32) * FACTOR_DOWN
    factor = jnp.concatenate([factor, jnp.zeros_like(factor)], axis=0)
    factor = lax.dot(pick_factor, factor, precision=lax.Precision.HIGHEST, preferred_element_type=F32)

    for c in range(forward.shape[0]):
        w = [message[pl.ds(2 * c + t, count, stride=per), :] for t in range(2)]
        byte = [lambda w: w & 255, lambda w: lax.shift_right_logical(w, 8) & 255, lambda w: lax.shift_right_logical(w, 16) & 255]
        parts = [[(f(v) - 128) for v in w] for f in byte] + [[lax.shift_right_arithmetic(v, 24) for v in w]]
        parts = [[v.astype(F32).astype(jnp.bfloat16) for v in p] for p in parts]
        low = jnp.concatenate(parts[0] + parts[1], axis=1)
        high = jnp.concatenate(parts[2] + parts[3], axis=1)
        table = jnp.concatenate([low, high], axis=0)
        picked = lax.dot(pick, table, preferred_element_type=F32)
        forward[c] = picked * factor[:, c : c + 1]
    for n in (0, 2, 3, 4):
        copies[n].wait()
    last = cells_x - 1
    below, above = below_above(far, near)
    prior_y, next_y = prior_next(first, second)
    for x in range(cells_x):
        e = strain_plane(
            v[0, x], v[0, x - 1] if x > 0 else below(0), next_y[0, x : x + 1],
            v[1, x], v[1, x + 1] if x < last else above(0), prior_y[0, x : x + 1],
            v[2, x], v[2, x + 1] if x < last else above(1), next_y[1, x : x + 1],
        )
        new = stress_plane([stress[k, x] for k in range(6)], e, lam[x], mu[x])
        for k in range(6):
            strain2[k, x] = e[k]
            stress[k, x] = new[k]
    results = load(((stress, out.at[pl.ds(3, 6)]),), sems)
    copies[5].wait()
    for step, strain in enumerate((strain1, strain2)):
        f = [forward[6 * step + n] for n in range(6)]
        e = [strain[n].reshape(rows, cells_z) for n in range(6)]
        add_lambda = (e[0] + e[1] + e[2]) * (f[0] + f[1] + f[2])
        add_mu = 2.0 * (e[0] * f[0] + e[1] * f[1] + e[2] * f[2])
        grad_lambda = add_lambda if step == 0 else grad_lambda + add_lambda
        grad_mu = add_mu if step == 0 else grad_mu + add_mu
        grad_mu = grad_mu + e[3] * f[3] + e[4] * f[4] + e[5] * f[5]
    grads[0] = grad_lambda.reshape(cells_x, cells_y, cells_z)
    grads[1] = grad_mu.reshape(cells_x, cells_y, cells_z)
    results += load(((grads, out_grads),), sems.at[pl.ds(1, 1)])
    for copy in results:
        copy.wait()


def on_device(adjoint, buoyancy, lame_lambda, shear_mu, packed, scales, perm):
    cells_x, cells_y, cells_z = buoyancy.shape
    owners, comp, width = packed.shape[1], packed.shape[3], packed.shape[4]
    per = comp * width // 128

    def shape(*dims, dtype=F32):
        return jax.ShapeDtypeStruct(dims, dtype)

    def in_hbm(*values):
        return [pltpu.with_memory_space_constraint(value, pltpu.HBM) for value in values]

    def call(kernel, mebibytes, outs, args, in_specs=None, scratch=(), out_specs=None, aliases={}):
        return pl.pallas_call(
            kernel,
            out_shape=outs,
            in_specs=in_specs or [VMEM] * len(args),
            out_specs=out_specs or (VMEM,) * len(outs),
            scratch_shapes=scratch,
            compiler_params=pltpu.CompilerParams(vmem_limit_bytes=mebibytes << 20),
            input_output_aliases=aliases,
        )(*args)

    count_x = lax.axis_size("gx")
    count_y = lax.axis_size("gy")
    off_chip = [(x, x + 1 if x % 2 else x - 1) for x in range(1, count_x - 1)]
    on_chip = [(x, x ^ 1) for x in range(count_x)]
    pairs = [[(y, y + 1) for y in range(start, count_y - 1, 2)] for start in (0, 1)]
    pairs = [[*there, *((b, a) for a, b in there)] for there in pairs]

    def planes(*count):
        return shape(*count, cells_y, cells_z)

    def lines(count):
        return shape(count, cells_x, cells_z)

    def rooms(*sizes):
        return [pltpu.VMEM(size, F32) for size in sizes]

    def semaphores(*counts):
        return [pltpu.SemaphoreType.DMA((count,)) for count in counts]

    raw = in_hbm(adjoint, buoyancy, lame_lambda, shear_mu)
    first, second = call(
        prepare, 8, (lines(len(UP_ROWS)), lines(len(UP_ROWS))), raw, [ANY] * 4, rooms((2, 12, cells_x, 8, cells_z)) + semaphores(8)
    )
    first = lax.ppermute(first, "gy", pairs[0])
    second = lax.ppermute(second, "gy", pairs[1])

    by_comp = jnp.transpose(scales.reshape(owners, comp)).reshape(comp, 1, owners)
    size = (owners * (per + 1), 128)
    (message,) = call(
        merge, 8, (pltpu.HBM(size, jnp.int32),), (*in_hbm(packed.reshape(owners * per, 128)), by_comp), [ANY, VMEM],
        [
            pltpu.VMEM((owners * per, 128), jnp.int32), pltpu.VMEM(size, jnp.int32),
            pltpu.SemaphoreType.DMA((4,)), pltpu.SemaphoreType.DMA((4,)),
        ],
        (ANY,),
    )
    message = lax.all_to_all(message.reshape(owners, per + 1, 1, 128), "gx", split_axis=0, concat_axis=0, tiled=True)
    message = message.reshape(owners * (per + 1), 128)

    whole = adjoint.shape
    strain = (6, *buoyancy.shape)
    speeds = (3, *buoyancy.shape)
    message_rows = (PLANES * cells_y + 8, cells_z)
    faces = shape(*message_rows)
    far, near = call(
        reach, 12, (faces, faces), (adjoint, buoyancy, *raw[2:], first, second), [VMEM] * 2 + [ANY] * 2 + [VMEM] * 2,
        rooms((3, cells_y, cells_z)) + semaphores(3),
    )
    far = lax.ppermute(far, "gx", off_chip)
    near = lax.ppermute(near, "gx", on_chip)

    fields, strain1, far, near, first, second = call(
        middle, 16, (pltpu.HBM(whole, F32), pltpu.HBM(strain, F32), planes(2), planes(2), lines(2), lines(2)),
        (*raw, far, near, first, second), [ANY] * 4 + [VMEM] * 4,
        rooms(whole, *[buoyancy.shape] * 3, speeds, strain, strain) + semaphores(4, 3), (ANY, ANY, VMEM, VMEM, VMEM, VMEM),
    )
    w_ghosts = (
        lax.ppermute(far, "gx", off_chip), lax.ppermute(near, "gx", on_chip),
        lax.ppermute(first, "gy", pairs[0]), lax.ppermute(second, "gy", pairs[1]),
    )
    grads = (2, *buoyancy.shape)
    adjoint_out, grads = call(
        finish, 24, (pltpu.HBM(whole, F32), pltpu.HBM(grads, F32)),
        (*in_hbm(fields, lame_lambda, shear_mu, strain1, perm), *w_ghosts, message), [ANY] * 5 + [VMEM] * 5,
        rooms(speeds, strain, buoyancy.shape, buoyancy.shape, strain) + [pltpu.VMEM(perm.shape, jnp.int32)]
        + rooms(strain, (comp, cells_x * cells_y, cells_z), grads) + semaphores(6, 2),
        (ANY, ANY), {0: 0},
    )
    return adjoint_out, grads


def solution(mesh):
    return jax.shard_map(
        on_device,
        mesh=mesh,
        in_specs=(
            P(None, "gx", "gy", None),
            P("gx", "gy", None),
            P("gx", "gy", None),
            P("gx", "gy", None),
            P("gx", None, "gy", None, None),
            P("gx", None, "gy", None),
            P("gx", None),
        ),
        out_specs=(P(None, "gx", "gy", None), P(None, "gx", "gy", None)),
        check_vma=False,
    )
```

```python
import jax
import jax.numpy as jnp
from jax import lax
from jax.experimental import pallas as pl
from jax.experimental.pallas import tpu as pltpu
from jax.sharding import PartitionSpec as P


courant = 0.15
FACTOR_UP = 2.0**35
FACTOR_DOWN = 2.0**-35
F32 = jnp.float32
ANY = pl.BlockSpec(memory_space=pl.ANY)
VMEM = pl.BlockSpec(memory_space=pltpu.VMEM)


def below_y(field, row):
    y = lax.broadcasted_iota(jnp.int32, field.shape, 0)
    return jnp.where(y == 0, row, pltpu.roll(field, 1, 0))


def above_y(field, row):
    count = field.shape[0]
    y = lax.broadcasted_iota(jnp.int32, field.shape, 0)
    return jnp.where(y == count - 1, row, pltpu.roll(field, count - 1, 0))


def below_z(field):
    z = lax.broadcasted_iota(jnp.int32, field.shape, 1)
    return jnp.where(z == 0, 0.0, pltpu.roll(field, 1, 1))


def above_z(field):
    count = field.shape[1]
    z = lax.broadcasted_iota(jnp.int32, field.shape, 1)
    return jnp.where(z == count - 1, 0.0, pltpu.roll(field, count - 1, 1))


def velocity_plane(vel, scaled, sxx, sxx_next, syy, syy_row, szz, sxy, sxy_prior, sxy_row, sxz, sxz_prior, syz, syz_row):
    vx, vy, vz = vel
    vx = vx - scaled * (sxx_next - sxx + (sxy - below_y(sxy, sxy_row)) + (sxz - below_z(sxz)))
    vy = vy - scaled * (sxy - sxy_prior + (above_y(syy, syy_row) - syy) + (syz - below_z(syz)))
    vz = vz - scaled * (sxz - sxz_prior + (syz - below_y(syz, syz_row)) + (above_z(szz) - szz))
    return vx, vy, vz


def strain_plane(vx, vx_prior, vx_row, vy, vy_next, vy_row, vz, vz_next, vz_row):
    exx = vx - vx_prior
    eyy = vy - below_y(vy, vy_row)
    ezz = vz - below_z(vz)
    exy = (above_y(vx, vx_row) - vx) + (vy_next - vy)
    exz = (above_z(vx) - vx) + (vz_next - vz)
    eyz = (above_z(vy) - vy) + (above_y(vz, vz_row) - vz)
    return exx, eyy, ezz, exy, exz, eyz


def stress_plane(stress, strain, lam, mu):
    trace = strain[0] + strain[1] + strain[2]
    direct = [stress[k] - courant * (lam * trace + 2.0 * mu * strain[k]) for k in range(3)]
    shear = [stress[k] - courant * mu * strain[k] for k in range(3, 6)]
    return direct + shear


UP_ROWS = tuple((n, 1) for n in (0, 1, 2, 3, 4, 5, 6, 7, 8, 9, 11)) + ((6, 2), (8, 2))
DOWN_ROWS = tuple((n, 1) for n in range(12)) + ((4, 2),)
PLANES = 7


def on_lower_core():
    return lax.axis_index("gx") % 2 == 0


def below_above(far, near):
    lower = on_lower_core()
    return lambda k: jnp.where(lower, far[k], near[k]), lambda k: jnp.where(lower, near[k], far[k])


def far_near(up, down):
    lower = on_lower_core()
    return jnp.where(lower, down, up), jnp.where(lower, up, down)


def on_even_row():
    return lax.axis_index("gy") % 2 == 0


def prior_next(first, second):
    even = on_even_row()
    return jnp.where(even, second[...], first[...]), jnp.where(even, first[...], second[...])


def first_second(to_next, to_prior):
    even = on_even_row()
    return jnp.where(even, to_next, to_prior), jnp.where(even, to_prior, to_next)


def prepare(adj, buoy, lam, mu, first, second, rows, sems):
    cells_y = adj.shape[2]
    extra = (buoy, lam, mu)
    plans = []
    for side, start in enumerate((cells_y - 8, 0)):
        plans.append((adj.at[:, :, pl.ds(start, 8)], rows.at[side, pl.ds(0, 9)]))
        plans += [(extra[n].at[:, pl.ds(start, 8)], rows.at[side, 9 + n]) for n in range(3)]
    for copy in load(plans, sems):
        copy.wait()
    for k, ((up, up_depth), (down, down_depth)) in enumerate(zip(UP_ROWS, DOWN_ROWS)):
        first[k], second[k] = first_second(rows[0, up, :, 8 - up_depth, :], rows[1, down, :, down_depth - 1, :])


def merge(packed, scales, message, words, build, word_sems, sems):
    comp, _, count = scales.shape
    per = packed.shape[0] // count
    size = 16
    starts = range(0, count, size)
    loads = []
    for n, start in enumerate(starts):
        part = pl.ds(start * per, size * per)
        loads.append(pltpu.make_async_copy(packed.at[part], words.at[part], word_sems.at[n]))
        loads[-1].start()
    factor = jnp.pad(scales[:, 0, :], ((0, 128 - comp), (0, 128 - count)))
    factor = (jnp.transpose(factor)[:count] * FACTOR_UP).astype(jnp.int32)
    build[pl.ds(per, count, stride=per + 1), :] = factor
    copies = []
    for n, start in enumerate(starts):
        loads[n].wait()
        for r in range(per):
            build[pl.ds(start * (per + 1) + r, size, stride=per + 1), :] = words[pl.ds(start * per + r, size, stride=per), :]
        part = pl.ds(start * (per + 1), size * (per + 1))
        copies.append(pltpu.make_async_copy(build.at[part], message.at[part], sems.at[n]))
        copies[-1].start()
    for copy in copies:
        copy.wait()


def load(plans, sems):
    copies = [pltpu.make_async_copy(source, target, sems.at[n]) for n, (source, target) in enumerate(plans)]
    for copy in copies:
        copy.start()
    return copies


def step_one(adj, buoy, x, sxx_next, sxy_prior, sxz_prior, prior_y, next_y):
    row = slice(x, x + 1)
    return velocity_plane(
        (adj[0, x], adj[1, x], adj[2, x]), courant * buoy[x], adj[3, x], sxx_next, adj[4, x], next_y[4, 1][row], adj[5, x],
        adj[6, x], sxy_prior, prior_y[6, 1][row], adj[7, x], sxz_prior, adj[8, x], prior_y[8, 1][row],
    )


def named_rows(first, second):
    prior_y, next_y = prior_next(first, second)
    return {name: prior_y[k] for k, name in enumerate(UP_ROWS)}, {name: next_y[k] for k, name in enumerate(DOWN_ROWS)}


def places(cells_y):
    return [pl.ds(k * cells_y, cells_y) for k in range(PLANES)], [pl.ds(PLANES * cells_y + k, 1) for k in range(6)]


def reach(adj_in, buoy_in, lam, mu, first, second, far, near, adj, buoy, planes, sems):
    cells_x, cells_y = adj.shape[1:3]
    last = cells_x - 1
    needed = [(adj_in.at[:, x], adj.at[:, x]) for x in (0, last)] + [(buoy_in.at[x], buoy.at[x]) for x in (0, last)]
    needed += [(adj_in.at[n, x], adj.at[n, x]) for n, x in ((3, 1), (6, last - 1), (7, last - 1))]
    loads = load((*needed, (mu.at[last], planes.at[0]), (lam.at[0], planes.at[1]), (mu.at[0], planes.at[2])), sems)
    prior_y, next_y = named_rows(first, second)
    for copy in loads[:-3]:
        copy.wait()
    blank = jnp.zeros_like(adj[0, 0])
    up = [*step_one(adj, buoy, last, blank, adj[6, last - 1], adj[7, last - 1], prior_y, next_y), buoy[last], adj[6, last], adj[7, last]]
    down = [*step_one(adj, buoy, 0, adj[3, 1], blank, blank, prior_y, next_y), buoy[0], adj[3, 0]]
    own = {n: next_y[n, 1][last:] for n in range(10)}
    scaled_up = courant * own[9]
    sides = (own[6] - adj[6, last][cells_y - 1 :, :]) + (own[7] - below_z(own[7]))
    up_rows = [own[0] - scaled_up * (sides - own[3]), scaled_up]
    up_rows += [rows[n, 1][last:] for rows in (prior_y, next_y) for n in (6, 7)]
    own = {n: prior_y[n, 1][0:1] for n in range(10)}
    scaled_down = courant * own[9]
    sides = (adj[4, 0][0:1, :] - own[4]) + (own[8] - below_z(own[8]))
    down_rows = [own[1] - scaled_down * (own[6] + sides), scaled_down, own[3], next_y[3, 1][0:1]]
    down_rows += [jnp.zeros_like(scaled_down)] * 2
    whole, lines = places(cells_y)
    for copy in loads[-3:]:
        copy.wait()
    up.append(planes[0])
    down += [planes[1], planes[2]]
    for place, a, b in zip(whole + lines, up + up_rows, down + down_rows):
        far[place, :], near[place, :] = far_near(a, b)


def half(adj, buoy, lam, mu, far, near, first, second, v, stress, strain, between):
    cells_x, cells_y = adj.shape[1:3]
    last = cells_x - 1
    from_below, from_above = below_above(far, near)
    prior_y, next_y = named_rows(first, second)
    whole, lines = places(cells_y)
    vx_m, vy_m, vz_m, buoy_m, sxy_m, sxz_m, mu_m = (from_below(place) for place in whole)
    vx_n, vy_n, vz_n, buoy_n, sxx_n, lam_n, mu_n = (from_above(place) for place in whole)
    vx_m = vx_m - courant * buoy_m * adj[3, 0]
    vy_n = vy_n + courant * buoy_n * adj[6, last]
    vz_n = vz_n + courant * buoy_n * adj[7, last]
    for x in range(cells_x):
        new = step_one(
            adj, buoy, x, adj[3, x + 1] if x < last else sxx_n, adj[6, x - 1] if x > 0 else sxy_m, adj[7, x - 1] if x > 0 else sxz_m,
            prior_y, next_y,
        )
        for k in range(3):
            v[k, x] = new[k]
    vx_corner = from_below(lines[0]) - from_below(lines[1]) * next_y[3, 1][0:1]
    vy_corner = from_above(lines[0]) + from_above(lines[1]) * prior_y[6, 1][last:]
    ghosts = []
    for side, here in enumerate((prior_y, next_y)):
        scaled = courant * here[9, 1]
        sxx, syy, szz, sxy, sxz, syz = (here[n, 1] for n in range(3, 9))
        sxx_after = jnp.concatenate([sxx[1:], from_above(lines[2 + side])], axis=0)
        sxy_before = jnp.concatenate([from_below(lines[2 + 2 * side]), sxy[:last]], axis=0)
        sxz_before = jnp.concatenate([from_below(lines[3 + 2 * side]), sxz[:last]], axis=0)
        if side == 0:
            sxy_under, syz_under, syy_over = here[6, 2], here[8, 2], adj[4, :, 0, :]
        else:
            sxy_under, syz_under, syy_over = adj[6, :, cells_y - 1, :], adj[8, :, cells_y - 1, :], here[4, 2]
        ghosts.append([
            here[0, 1] - scaled * (sxx_after - sxx + (sxy - sxy_under) + (sxz - below_z(sxz))),
            here[1, 1] - scaled * (sxy - sxy_before + (syy_over - syy) + (syz - below_z(syz))),
            here[2, 1] - scaled * (sxz - sxz_before + (syz - syz_under) + (above_z(szz) - szz)),
        ])
    v_prior_y, v_next_y = ghosts
    exx = vx_n - v[0, last]
    trace = exx + (vy_n - below_y(vy_n, vy_corner)) + (vz_n - below_z(vz_n))
    sxx_next = sxx_n - courant * (lam_n * trace + 2.0 * mu_n * exx)
    exy = (above_y(vx_m, vx_corner) - vx_m) + (v[1, 0] - vy_m)
    exz = (above_z(vx_m) - vx_m) + (v[2, 0] - vz_m)
    sxy_prior = sxy_m - courant * mu_m * exy
    sxz_prior = sxz_m - courant * mu_m * exz
    over = v_next_y[0]
    exx = over - jnp.concatenate([vx_corner, over[:last]], axis=0)
    eyy = v_next_y[1] - v[1, :, cells_y - 1, :]
    trace = exx + eyy + (v_next_y[2] - below_z(v_next_y[2]))
    syy_rows = next_y[4, 1] - courant * (next_y[10, 1] * trace + 2.0 * next_y[11, 1] * eyy)
    under = v_prior_y[1]
    exy = (v[0, :, 0, :] - v_prior_y[0]) + (jnp.concatenate([under[1:], vy_corner], axis=0) - under)
    eyz = (above_z(under) - under) + (v[2, :, 0, :] - v_prior_y[2])
    sxy_rows = prior_y[6, 1] - courant * prior_y[11, 1] * exy
    syz_rows = prior_y[8, 1] - courant * prior_y[11, 1] * eyz
    for x in range(cells_x):
        e = strain_plane(
            v[0, x], v[0, x - 1] if x > 0 else vx_m, v_next_y[0][x : x + 1],
            v[1, x], v[1, x + 1] if x < last else vy_n, v_prior_y[1][x : x + 1],
            v[2, x], v[2, x + 1] if x < last else vz_n, v_next_y[2][x : x + 1],
        )
        s = stress_plane([adj[3 + k, x] for k in range(6)], e, lam[x], mu[x])
        for k in range(6):
            stress[k, x] = s[k]
            if strain is not None:
                strain[k, x] = e[k]
    between()
    for x in range(cells_x):
        new = velocity_plane(
            (v[0, x], v[1, x], v[2, x]), courant * buoy[x],
            stress[0, x], stress[0, x + 1] if x < last else sxx_next, stress[1, x], syy_rows[x : x + 1], stress[2, x],
            stress[3, x], stress[3, x - 1] if x > 0 else sxy_prior, sxy_rows[x : x + 1],
            stress[4, x], stress[4, x - 1] if x > 0 else sxz_prior, stress[5, x], syz_rows[x : x + 1],
        )
        for k in range(3):
            v[k, x] = new[k]


def middle(
    adj_in, buoy_in, lam_in, mu_in, far_in, near_in, first_in, second_in, fields, strain_out, far, near, first, second,
    adj, buoy, lam, mu, v, stress, strain, load_sems, sems,
):
    here = (adj, buoy, lam, mu)
    for copy in load(zip((adj_in, buoy_in, lam_in, mu_in), here), load_sems):
        copy.wait()
    copies = [
        pltpu.make_async_copy(strain, strain_out, sems.at[0]),
        pltpu.make_async_copy(stress, fields.at[pl.ds(3, 6)], sems.at[1]),
        pltpu.make_async_copy(v, fields.at[pl.ds(0, 3)], sems.at[2]),
    ]
    half(*here, far_in, near_in, first_in, second_in, v, stress, strain, lambda: [copy.start() for copy in copies[:2]])
    copies[2].start()
    _, cells_x, cells_y, _ = v.shape
    over, under = v[1, :, cells_y - 1, :], v[0, :, 0, :]
    first[0], second[0] = first_second(over, under)
    under = v[2, :, 0, :]
    first[1], second[1] = first_second(jnp.zeros_like(under), under)
    far[0], near[0] = far_near(v[0, cells_x - 1], v[1, 0])
    far[1], near[1] = far_near(jnp.zeros_like(v[2, 0]), v[2, 0])
    for copy in copies:
        copy.wait()


def finish(
    fields, lam_in, mu_in, strain_in, perm_in, far, near, first, second, message, out, out_grads,
    v, stress, lam, mu, strain1, perm, strain2, forward, grads, load_sems, sems,
):
    cells_x, cells_y, cells_z = strain1.shape[1:]
    plans = (
        (fields.at[pl.ds(0, 3)], v), (perm_in, perm), (fields.at[pl.ds(3, 6)], stress), (lam_in, lam), (mu_in, mu), (strain_in, strain1),
    )
    copies = load(plans, load_sems)
    count = perm.shape[1]
    per = message.shape[0] // count
    rows = cells_x * cells_y
    copies[1].wait()
    both = jnp.concatenate([perm[...], perm[...]], axis=1)
    r = lax.broadcasted_iota(jnp.int32, (rows, 2 * count), 0)
    k = lax.broadcasted_iota(jnp.int32, (rows, 2 * count), 1)
    mine = both == lax.shift_right_logical(r, 1)
    half = (k >= count) == ((r & 1) == 1)
    pick = jnp.where(mine & half, 1.0, 0.0).astype(jnp.bfloat16)
    pick_factor = jnp.where(mine & (k < count), 1.0, 0.0)
    factor = message[pl.ds(per - 1, count, stride=per), :].astype(F32) * FACTOR_DOWN
    factor = jnp.concatenate([factor, jnp.zeros_like(factor)], axis=0)
    factor = lax.dot(pick_factor, factor, precision=lax.Precision.HIGHEST, preferred_element_type=F32)

    for c in range(forward.shape[0]):
        w = [message[pl.ds(2 * c + t, count, stride=per), :] for t in range(2)]
        byte = [lambda w: w & 255, lambda w: lax.shift_right_logical(w, 8) & 255, lambda w: lax.shift_right_logical(w, 16) & 255]
        parts = [[(f(v) - 128) for v in w] for f in byte] + [[lax.shift_right_arithmetic(v, 24) for v in w]]
        parts = [[v.astype(F32).astype(jnp.bfloat16) for v in p] for p in parts]
        low = jnp.concatenate(parts[0] + parts[1], axis=1)
        high = jnp.concatenate(parts[2] + parts[3], axis=1)
        table = jnp.concatenate([low, high], axis=0)
        picked = lax.dot(pick, table, preferred_element_type=F32)
        forward[c] = picked * factor[:, c : c + 1]
    for n in (0, 2, 3, 4):
        copies[n].wait()
    last = cells_x - 1
    below, above = below_above(far, near)
    prior_y, next_y = prior_next(first, second)
    for x in range(cells_x):
        e = strain_plane(
            v[0, x], v[0, x - 1] if x > 0 else below(0), next_y[0, x : x + 1],
            v[1, x], v[1, x + 1] if x < last else above(0), prior_y[0, x : x + 1],
            v[2, x], v[2, x + 1] if x < last else above(1), next_y[1, x : x + 1],
        )
        new = stress_plane([stress[k, x] for k in range(6)], e, lam[x], mu[x])
        for k in range(6):
            strain2[k, x] = e[k]
            stress[k, x] = new[k]
    results = load(((stress, out.at[pl.ds(3, 6)]),), sems)
    copies[5].wait()
    for step, strain in enumerate((strain1, strain2)):
        f = [forward[6 * step + n] for n in range(6)]
        e = [strain[n].reshape(rows, cells_z) for n in range(6)]
        add_lambda = (e[0] + e[1] + e[2]) * (f[0] + f[1] + f[2])
        add_mu = 2.0 * (e[0] * f[0] + e[1] * f[1] + e[2] * f[2])
        grad_lambda = add_lambda if step == 0 else grad_lambda + add_lambda
        grad_mu = add_mu if step == 0 else grad_mu + add_mu
        grad_mu = grad_mu + e[3] * f[3] + e[4] * f[4] + e[5] * f[5]
    grads[0] = grad_lambda.reshape(cells_x, cells_y, cells_z)
    grads[1] = grad_mu.reshape(cells_x, cells_y, cells_z)
    results += load(((grads, out_grads),), sems.at[pl.ds(1, 1)])
    for copy in results:
        copy.wait()


def on_device(adjoint, buoyancy, lame_lambda, shear_mu, packed, scales, perm):
    cells_x, cells_y, cells_z = buoyancy.shape
    owners, comp, width = packed.shape[1], packed.shape[3], packed.shape[4]
    per = comp * width // 128

    def shape(*dims, dtype=F32):
        return jax.ShapeDtypeStruct(dims, dtype)

    def in_hbm(*values):
        return [pltpu.with_memory_space_constraint(value, pltpu.HBM) for value in values]

    def call(kernel, mebibytes, outs, args, in_specs=None, scratch=(), out_specs=None, aliases={}):
        return pl.pallas_call(
            kernel,
            out_shape=outs,
            in_specs=in_specs or [VMEM] * len(args),
            out_specs=out_specs or (VMEM,) * len(outs),
            scratch_shapes=scratch,
            compiler_params=pltpu.CompilerParams(vmem_limit_bytes=mebibytes << 20),
            input_output_aliases=aliases,
        )(*args)

    count_x = lax.axis_size("gx")
    count_y = lax.axis_size("gy")
    off_chip = [(x, x + 1 if x % 2 else x - 1) for x in range(1, count_x - 1)]
    on_chip = [(x, x ^ 1) for x in range(count_x)]
    pairs = [[(y, y + 1) for y in range(start, count_y - 1, 2)] for start in (0, 1)]
    pairs = [[*there, *((b, a) for a, b in there)] for there in pairs]

    def planes(*count):
        return shape(*count, cells_y, cells_z)

    def lines(count):
        return shape(count, cells_x, cells_z)

    def rooms(*sizes):
        return [pltpu.VMEM(size, F32) for size in sizes]

    def semaphores(*counts):
        return [pltpu.SemaphoreType.DMA((count,)) for count in counts]

    raw = in_hbm(adjoint, buoyancy, lame_lambda, shear_mu)
    first, second = call(
        prepare, 8, (lines(len(UP_ROWS)), lines(len(UP_ROWS))), raw, [ANY] * 4, rooms((2, 12, cells_x, 8, cells_z)) + semaphores(8)
    )
    first = lax.ppermute(first, "gy", pairs[0])
    second = lax.ppermute(second, "gy", pairs[1])

    by_comp = jnp.transpose(scales.reshape(owners, comp)).reshape(comp, 1, owners)
    size = (owners * (per + 1), 128)
    (message,) = call(
        merge, 8, (pltpu.HBM(size, jnp.int32),), (*in_hbm(packed.reshape(owners * per, 128)), by_comp), [ANY, VMEM],
        [
            pltpu.VMEM((owners * per, 128), jnp.int32), pltpu.VMEM(size, jnp.int32),
            pltpu.SemaphoreType.DMA((4,)), pltpu.SemaphoreType.DMA((4,)),
        ],
        (ANY,),
    )
    message = lax.all_to_all(message.reshape(owners, per + 1, 1, 128), "gx", split_axis=0, concat_axis=0, tiled=True)
    message = message.reshape(owners * (per + 1), 128)

    whole = adjoint.shape
    strain = (6, *buoyancy.shape)
    speeds = (3, *buoyancy.shape)
    message_rows = (PLANES * cells_y + 8, cells_z)
    faces = shape(*message_rows)
    far, near = call(
        reach, 12, (faces, faces), (*raw, first, second), [ANY] * 4 + [VMEM] * 2,
        rooms(whole, buoyancy.shape, (3, cells_y, cells_z)) + semaphores(10),
    )
    far = lax.ppermute(far, "gx", off_chip)
    near = lax.ppermute(near, "gx", on_chip)

    fields, strain1, far, near, first, second = call(
        middle, 16, (pltpu.HBM(whole, F32), pltpu.HBM(strain, F32), planes(2), planes(2), lines(2), lines(2)),
        (*raw, far, near, first, second), [ANY] * 4 + [VMEM] * 4,
        rooms(whole, *[buoyancy.shape] * 3, speeds, strain, strain) + semaphores(4, 3), (ANY, ANY, VMEM, VMEM, VMEM, VMEM),
    )
    w_ghosts = (
        lax.ppermute(far, "gx", off_chip), lax.ppermute(near, "gx", on_chip),
        lax.ppermute(first, "gy", pairs[0]), lax.ppermute(second, "gy", pairs[1]),
    )
    grads = (2, *buoyancy.shape)
    adjoint_out, grads = call(
        finish, 24, (pltpu.HBM(whole, F32), pltpu.HBM(grads, F32)),
        (*in_hbm(fields, lame_lambda, shear_mu, strain1, perm), *w_ghosts, message), [ANY] * 5 + [VMEM] * 5,
        rooms(speeds, strain, buoyancy.shape, buoyancy.shape, strain) + [pltpu.VMEM(perm.shape, jnp.int32)]
        + rooms(strain, (comp, cells_x * cells_y, cells_z), grads) + semaphores(6, 2),
        (ANY, ANY), {0: 0},
    )
    return adjoint_out, grads


def solution(mesh):
    return jax.shard_map(
        on_device,
        mesh=mesh,
        in_specs=(
            P(None, "gx", "gy", None),
            P("gx", "gy", None),
            P("gx", "gy", None),
            P("gx", "gy", None),
            P("gx", None, "gy", None, None),
            P("gx", None, "gy", None),
            P("gx", None),
        ),
        out_specs=(P(None, "gx", "gy", None), P(None, "gx", "gy", None)),
        check_vma=False,
    )
```
